32 devices in a mesh: emb: 4 (over x, core), seq: 8 (over z, y).
Axes of the slice: x: 2, y: 2, z: 4, core: 2. Of those that a mesh axis runs over, the one named last changes fastest.
Arguments:
- token_rows: int32 [4, 4096], P('emb', 'seq'), may hold values from 0 to 4223, as said below
- segment_ids: int32 [4, 4096], P('emb', 'seq'), may hold values from 0 to 3, never falling along the last dimension, each value on 1 to 2048 neighbouring positions
- requests: int32 [32, 32, 4], P(('emb', 'seq')), may hold values from 0 to 8191, as said below
- hot_table: bfloat16 [4096, 512], replicated, may hold values from -6 to 6
- cold_table: bfloat16 [262144, 512], P(('emb', 'seq')), may hold values from -6 to 6
- input_weight: bfloat16 [512, 2048], replicated, may hold values from -0.75 to 0.75
- output_weight: bfloat16 [512, 512], replicated, may hold values from -0.25 to 0.25
- up_weight: bfloat16 [512, 2048], replicated, may hold values from -0.25 to 0.25
- down_weight: bfloat16 [2048, 512], replicated, may hold values from -0.125 to 0.125
Outputs:
- layer_output: bfloat16 [4, 4096, 512], P('emb', 'seq')
The draws below stay inside these ranges and needn't reach their ends.
Inputs may be any that keep to these rules, and one draw needn't show every extreme that they name: `token_rows`: A value below 4096 names that row of hot_table. A value 4096 + o * 4 + k names slot k of the holding device's requests to owner o, and that slot is always a live one. Exactly 256 positions of each device name request slots. For each requesting device and owner the live requests fill slots 0 to c - 1, with c from 1 to 4; dead slots hold 0. Some owners, the same ones for all requesters, get all 4 slots live from every device, and every draw has at least one such owner. `segment_ids`: segment numbers never fall along a sequence.
All inputs are finite; a program needn't handle non-finite values.
Results may differ from the reference program's by a relative error of at most 0.0087.
Values may be sent and summed in bfloat16 or wider, within the bound.
No kernel may reach another device: no remote copies, remote signals or barrier semaphores. Data moves between devices by JAX's collectives and lax.ppermute only.
A program may use at most 128 MiB of HBM per device.

```python
import math
import jax
import jax.numpy as jnp
import numpy as np
from jax import lax

D = 512
H = 16
FF = 2048
HOT = 4096
COLD_DEV = 8192
CAP = 4
SEQ_DEV = 512
L = 4096
N_EMB = 4
N_SEQ = 8
DEVICES = 32


def plan_tokens(key):
    folded = jax.random.fold_in(key, 4099)
    subkeys = jax.random.split(folded, 6)
    owners = jnp.arange(DEVICES, dtype=jnp.int32)
    heavy_owner = jax.random.randint(subkeys[0], (DEVICES,), 0, 4) == 0
    forced = jax.random.randint(subkeys[1], (), 0, DEVICES)
    heavy_owner = heavy_owner | (owners == forced)
    light_count = jax.random.randint(subkeys[2], (DEVICES, DEVICES), 1, CAP // 2 + 1)
    counts = jnp.where(heavy_owner[None, :], CAP, light_count)
    slot_index = jnp.arange(DEVICES * CAP, dtype=jnp.int32)
    live_slot = (slot_index % CAP)[None, :] < jnp.repeat(counts, CAP, axis=1)
    wanted = jax.random.randint(subkeys[3], (DEVICES, DEVICES * CAP), 0, COLD_DEV)
    requests = jnp.where(live_slot, wanted, 0).reshape(DEVICES, DEVICES, CAP).astype(jnp.int32)
    live_order = jnp.argsort(1 - live_slot.astype(jnp.int32), axis=1, stable=True).astype(jnp.int32)
    live_total = jnp.sum(live_slot.astype(jnp.int32), axis=1)
    shuffle_keys = jax.random.randint(subkeys[4], (DEVICES, SEQ_DEV), 0, 1 << 20) * SEQ_DEV + jnp.arange(SEQ_DEV, dtype=jnp.int32)[None, :]
    token_rank = jnp.argsort(jnp.argsort(shuffle_keys, axis=1, stable=True), axis=1, stable=True).astype(jnp.int32)
    is_cold = token_rank < SEQ_DEV // 2
    picked = jnp.take_along_axis(live_order, token_rank % live_total[:, None], axis=1)
    hot_choice = jax.random.randint(subkeys[5], (DEVICES, SEQ_DEV), 0, HOT)
    item_ids = jnp.where(is_cold, HOT + picked, hot_choice).astype(jnp.int32)
    return (requests, item_ids.reshape(N_EMB, SEQ_DEV * N_SEQ))


def draw_token_rows(key, part):
    return plan_tokens(key)[1]


def draw_requests(key, part):
    return plan_tokens(key)[0]


def levels(key, extent, cuts, low, largest):
    loudness, own = 1.0, jax.random.fold_in(key, 6)
    for dim, blocks in cuts:
        heights = jnp.exp(jax.random.uniform(jax.random.fold_in(own, dim), (blocks,), jnp.float32, low / len(cuts), largest / len(cuts)))
        loudness = loudness * jnp.repeat(heights, extent[dim] // blocks).reshape([-1 if axis == dim else 1 for axis in range(len(extent))])
    return loudness


def length_profile(count, total, reach, slope):
    portions = [(1 << 20) // math.isqrt(rank ** slope) + 1 for rank in range(2, count + 1)]
    surplus, holding = total - reach - (count - 1), [1] * (count - 1)
    while surplus > 0:
        free = [i for i in range(count - 1) if holding[i] < reach]
        whole, budget = sum([portions[i] for i in free]), surplus
        for i in free:
            more = min(reach - holding[i], max(1, budget * portions[i] // whole), surplus)
            holding[i] = holding[i] + more
            surplus = surplus - more
    return np.array([reach] + holding)


def ragged(rng, amount, total, most, skew):
    if amount == 2:
        one = jax.random.randint(rng, (), max(1, total - most), min(most, total - 1) + 1)
        return jnp.stack([one, total - one])
    lengths = jnp.asarray(length_profile(amount, total, most, skew), jnp.int32)
    pairs = (amount - 1) // 2
    giver, receiver = lengths[1:1 + 2 * pairs:2], lengths[2:2 + 2 * pairs:2]
    room = jnp.minimum(giver - 1, most - receiver)
    moved = jax.random.randint(jax.random.fold_in(rng, 1), (pairs,), 0, 1 << 20) % (room + 1)
    lengths = lengths.at[1:1 + 2 * pairs:2].set(giver - moved).at[2:2 + 2 * pairs:2].set(receiver + moved)
    return lengths[jax.random.permutation(jax.random.fold_in(rng, 2), amount)]


def noise(rng, shape, width, reach, pieces=(), kind=jnp.bfloat16):
    values = jax.random.normal(rng, shape, jnp.float32) * width
    if len(pieces) > 0:
        values = levels(rng, shape, pieces, -0.22, 0.18) * values
    return jnp.clip(values, min=-reach, max=reach).astype(kind)


def setup_inputs(seed: int = 0) -> dict:
    streams_of = jax.random.split(jax.random.key(seed), 10)
    return {
        "token_rows": draw_token_rows(jax.random.fold_in(streams_of[9], 71), 0),
        "segment_ids": jax.vmap(lambda own: jnp.searchsorted(jnp.cumsum(ragged(own, 4, L, L // 2, 0)), jnp.arange(L), side="right"))(jax.random.split(streams_of[1], N_EMB)).reshape((N_EMB, L)).astype(jnp.int32),
        "requests": draw_requests(jax.random.fold_in(streams_of[9], 71), 0),
        "hot_table": noise(streams_of[3], (HOT, D), 1.0, 6.0),
        "cold_table": noise(streams_of[4], (DEVICES * COLD_DEV, D), 1.0, 6.0, ((0, 32),)),
        "input_weight": noise(streams_of[5], (D, 4 * D), (D // 9) ** -0.5, 0.75),
        "output_weight": noise(streams_of[6], (D, D), D ** -0.5, 0.25),
        "up_weight": noise(streams_of[7], (D, FF), D ** -0.5, 0.25),
        "down_weight": noise(streams_of[8], (FF, D), FF ** -0.5, 0.125),
    }


epsilon = 1e-06

def normalize(values):
    widened = values.astype(jnp.float32)
    return widened * lax.rsqrt(lax.optimization_barrier(jnp.mean(widened * widened, axis=-1, keepdims=True)) + epsilon)

def reference(token_rows, segment_ids, requests, hot_table, cold_table, input_weight, output_weight, up_weight, down_weight):
    length = SEQ_DEV * N_SEQ
    block_rows = math.gcd(length, 1024)
    blocks = length // block_rows
    head_width = D // H
    score_scale = 1.0 / math.sqrt(head_width)
    flat_requests = requests.reshape(DEVICES, DEVICES * CAP)
    places = jnp.arange(length, dtype=jnp.int32)
    offsets = jnp.arange(block_rows, dtype=jnp.int32)

    def one_sequence(inputs):
        item_ids, segments, member = inputs
        device = member * N_SEQ + places // SEQ_DEV
        is_hot = item_ids < HOT
        slot_index = jnp.where(is_hot, 0, item_ids - HOT)
        local_row = flat_requests[device, slot_index]
        cold_rows = cold_table[slot_index // CAP * COLD_DEV + local_row]
        hot_rows = hot_table[jnp.where(is_hot, item_ids, 0)]
        embedded = jnp.where(is_hot[:, None], hot_rows, cold_rows)
        normed_input = normalize(embedded).astype(jnp.bfloat16)
        projected = jnp.dot(normed_input, input_weight, preferred_element_type=jnp.float32).astype(jnp.bfloat16)
        projected = lax.optimization_barrier(projected).reshape(length, H, 4, head_width)
        gate_units = jax.nn.silu(projected[:, :, 0].astype(jnp.float32)).reshape(length, D)
        heads_first = jnp.moveaxis(projected[:, :, 1:], 1, 0)

        def one_head(head_rows):
            value_rows = head_rows[:, 0].astype(jnp.float32)
            query_rows = head_rows[:, 1].astype(jnp.float32)
            key_rows = head_rows[:, 2].astype(jnp.float32)

            def one_block(block_inputs):
                query_block, query_segments, position = block_inputs
                query_places = position * block_rows + offsets
                scores = jnp.dot(query_block, key_rows.T, preferred_element_type=jnp.float32) * score_scale
                allowed = (places[None, :] <= query_places[:, None]) & (query_segments[:, None] == segments[None, :])
                weights = jnp.where(allowed, jax.nn.silu(scores), 0.0).astype(jnp.bfloat16)
                weights = lax.optimization_barrier(weights).astype(jnp.float32)
                return jnp.dot(weights, value_rows, preferred_element_type=jnp.float32).astype(jnp.bfloat16)
            outputs = lax.map(one_block, (query_rows.reshape(blocks, block_rows, head_width), segments.reshape(blocks, block_rows), jnp.arange(blocks, dtype=jnp.int32)))
            return outputs.reshape(length, head_width)
        attended = lax.map(one_head, heads_first)
        attended = jnp.moveaxis(attended, 0, 1).reshape(length, D).astype(jnp.float32)
        mean_square = lax.optimization_barrier(jnp.mean(attended * attended, axis=-1, keepdims=True))
        normed_heads = (attended * lax.rsqrt(mean_square + epsilon) * gate_units).astype(jnp.bfloat16)
        hidden = embedded.astype(jnp.float32) + jnp.dot(normed_heads, output_weight, preferred_element_type=jnp.float32)
        normed_hidden = normalize(hidden).astype(jnp.bfloat16)
        activated = jax.nn.silu(jnp.dot(normed_hidden, up_weight, preferred_element_type=jnp.float32)).astype(jnp.bfloat16)
        return (hidden + jnp.dot(activated, down_weight, preferred_element_type=jnp.float32)).astype(jnp.bfloat16)
    return lax.map(one_sequence, (token_rows, segment_ids, jnp.arange(N_EMB, dtype=jnp.int32)))
```

```python
import functools
import math

import jax
import jax.numpy as jnp
from jax import lax
from jax.experimental import pallas as pl
from jax.experimental.pallas import tpu as pltpu
from jax.sharding import PartitionSpec as P

H = 16
LANES = 128
PICK = 8
SEGMENTS = 4
epsilon = 1e-06
f32 = jnp.float32
bf16 = jnp.bfloat16

VMEM = pl.BlockSpec(memory_space=pltpu.VMEM)
SMEM = pl.BlockSpec(memory_space=pltpu.SMEM)
ANY = pl.BlockSpec(memory_space=pl.ANY)


def call(body, out_shape, in_specs, out_specs, scratch=(), flops=0, name=None, size=48):
    return pl.pallas_call(
        body,
        out_shape=out_shape,
        in_specs=in_specs,
        out_specs=out_specs,
        scratch_shapes=list(scratch),
        compiler_params=pltpu.CompilerParams(vmem_limit_bytes=size * 1024 * 1024),
        cost_estimate=pl.CostEstimate(flops=flops, bytes_accessed=0, transcendentals=0),
        name=name,
    )


def dot(a, b, ca, cb):
    return lax.dot_general(a, b, (((ca,), (cb,)), ((), ())), preferred_element_type=f32)


def silu(x):
    half = x * 0.5
    return half * jnp.tanh(half) + half


def rms(x, axis):
    return lax.rsqrt(jnp.mean(x * x, axis=axis, keepdims=True) + epsilon)


def owner_body(head_groups, emb, seq, cap, req, message, cold, weight, sent, rows, tiles, sem):
    count = emb * seq * cap
    per = LANES // cap

    def fetch(i, _):
        for k in range(cap):
            row = req[i, k]
            base = pl.multiple_of((row // PICK) * PICK, PICK)
            slot = pl.multiple_of((i * cap + k) * PICK, PICK)
            pltpu.make_async_copy(
                cold.at[pl.ds(base, PICK)], tiles.at[pl.ds(slot, PICK)], sem
            ).start()
        return 0

    lax.fori_loop(0, emb * seq, fetch, 0)
    tags = message[:, message.shape[1] - 2, :]
    parts = []
    pltpu.make_async_copy(cold.at[pl.ds(0, count * PICK)], tiles, sem).wait()
    for group in range(count // LANES):
        owner = lax.broadcasted_iota(jnp.int32, (per, LANES), 0)
        lane = lax.broadcasted_iota(jnp.int32, (per, LANES), 1)
        mine = jnp.where(lane // cap == owner, tags[group * per : (group + 1) * per], 0)
        wanted = jnp.sum(mine, axis=0, keepdims=True)
        place = lax.broadcasted_iota(jnp.int32, (LANES * PICK, LANES), 0)
        column = lax.broadcasted_iota(jnp.int32, (1, LANES), 1)
        pick = (place == column * PICK + wanted % PICK).astype(f32).astype(bf16)
        block = tiles[group * LANES * PICK : (group + 1) * LANES * PICK]
        parts.append(dot(pick, block, 0, 0))
    for group, part in enumerate(parts):
        rows[group * LANES : (group + 1) * LANES] = part.astype(bf16)
        normed = (part * rms(part, 1)).astype(bf16)
        projected = dot(normed, weight[...], 1, 0).astype(bf16)
        span = seq * cap
        for local in range(LANES // span):
            member = group * (LANES // span) + local
            for g in range(seq):
                piece = projected[local * span : (local + 1) * span]
                if head_groups == 1:
                    sent[member * seq + g] = piece[:, g * LANES : (g + 1) * LANES]
                else:
                    low = piece[:, (2 * g) * LANES : (2 * g + 1) * LANES]
                    high = piece[:, (2 * g + 1) * LANES : (2 * g + 2) * LANES]
                    sent[member * seq + g, :span] = jnp.concatenate(
                        [high[:, 32:64], low[:, 32:]], axis=1
                    )
                    sent[member * seq + g, span:] = jnp.concatenate(
                        [high[span // 2 :, 64:], high[: span // 2, 64:]], axis=1
                    )


def hot_body(head_groups, table, weight, out):
    x = table[...].astype(f32)
    normed = (x * rms(x, 1)).astype(bf16)
    flat = dot(weight[...], normed, 0, 1).astype(bf16)
    if head_groups == 1:
        out[...] = flat
    else:
        out[0:32] = flat[160:192]
        out[32:128] = flat[32:128]
        out[128:192] = flat[192:256]


def spread_body(step, ids, table, out):
    tokens = ids.shape[2]
    hot = table.shape[1]
    own = ids[0]

    def add(c, acc):
        start = pl.multiple_of(c * step, step)
        place = lax.broadcasted_iota(jnp.int32, (step, tokens), 0)
        pick = (place == own - start).astype(f32).astype(bf16)
        return acc + dot(table[:, pl.ds(start, step)], pick, 1, 0)

    out[...] = lax.fori_loop(
        0, hot // step, add, jnp.zeros(out.shape, f32), unroll=2
    ).astype(bf16)


def own_body(hot, ids_col, ids_row, table, fetched, weight, embedded, gates):
    tokens = ids_row.shape[1]
    place = lax.broadcasted_iota(jnp.int32, (fetched.shape[0], tokens), 0)
    pick = (place == ids_row[...] - hot).astype(f32).astype(bf16)
    emb = dot(pick, fetched[...], 0, 0) + table[...].astype(f32)
    embedded[...] = emb.astype(bf16)
    normed = (emb * rms(emb, 1)).astype(bf16)
    u = dot(weight[...], normed, 0, 1).astype(bf16).astype(f32)
    gates[...] = silu(u)


def hot_rows_body(step, ids_col, table, out):
    tokens = ids_col.shape[0]
    acc = jnp.zeros(out.shape, f32)
    for c in range(table.shape[0] // step):
        place = lax.broadcasted_iota(jnp.int32, (tokens, step), 1) + c * step
        pick = (place == ids_col[...]).astype(f32).astype(bf16)
        acc = acc + dot(pick, table[c * step : (c + 1) * step], 1, 0)
    out[...] = acc.astype(bf16)


def attend_body(
    head_groups, seq, cap, hot, width, bq, bk, starts, ids, table, got, out, qt, vt, kr
):
    tokens = ids.shape[1]
    length = seq * tokens
    owners = got.shape[0]
    quarter = 16 // cap
    span = seq * cap
    for part in range(span // 16):
        a = got[:, part * 16 : (part + 1) * 16, :].reshape(owners * 16, LANES)
        if head_groups == 1:
            lhs = a.astype(f32).T.astype(bf16)
        else:
            b = got[:, span:, :].reshape(owners * 16, LANES)
            b = b[:, 64:] if part == 0 else b[:, :64]
            lhs = jnp.concatenate([a.astype(f32).T, b.astype(f32).T], axis=0).astype(bf16)
        for within in range(quarter):
            s = part * quarter + within
            slot = ids[s : s + 1] - hot
            code = jnp.where(slot >= 0, (slot // cap) * 16 + within * cap + slot % cap, -1)
            place = lax.broadcasted_iota(jnp.int32, (owners * 16, tokens), 0)
            pick = (place == code).astype(f32).astype(bf16)
            at = slice(s * tokens, (s + 1) * tokens)
            full = dot(lhs, pick, 1, 0) + table[:, at].astype(f32)
            full_b = full.astype(bf16)
            if head_groups == 1:
                order = ((32, 64, 96),)
            else:
                order = ((32, 64, 96), (0, 128, 160))
            for h, (v, q, k) in enumerate(order):
                vt[h, :, at] = full_b[v : v + width]
                qt[h, :, at] = full_b[q : q + width]
                kr[h, at, :] = full[k : k + width].T.astype(bf16)
    scale = 0.5 / math.sqrt(width)
    edges = [starts[i] for i in range(1, SEGMENTS)]

    def begin(p):
        best = 0
        for edge in edges:
            best = jnp.where(p >= edge, edge, best)
        return best

    def one_query(qb, _):
        q0 = pl.multiple_of(qb * bq, bq)
        row = q0 + lax.broadcasted_iota(jnp.int32, (1, bq), 1)
        first = begin(row)
        low = begin(q0)
        high = begin(q0 + bq - 1)
        diagonal = q0 // bk
        queries = [qt[h, :, pl.ds(q0, bq)] for h in range(head_groups)]

        def add(kb, acc, masked):
            k0 = pl.multiple_of(kb * bk, bk)
            if masked:
                key = k0 + lax.broadcasted_iota(jnp.int32, (bk, bq), 0)
                keep = (key <= row) & (key >= first)
            result = []
            for h in range(head_groups):
                score = dot(kr[h, pl.ds(k0, bk), :], queries[h], 1, 0)
                half = score * scale
                weight = half * jnp.tanh(half) + half
                if masked:
                    weight = jnp.where(keep, weight, 0.0)
                result.append(acc[h] + dot(vt[h, :, pl.ds(k0, bk)], weight.astype(bf16), 1, 0))
            return tuple(result)

        acc = tuple(jnp.zeros((width, bq), f32) for _ in range(head_groups))
        from_block = low // bk
        clear = jnp.minimum((high + bk - 1) // bk, diagonal)
        clear = jnp.maximum(clear, from_block)
        acc = lax.fori_loop(from_block, clear, lambda i, a: add(i, a, True), acc)
        acc = lax.fori_loop(clear, diagonal, lambda i, a: add(i, a, False), acc)
        acc = lax.fori_loop(
            jnp.maximum(diagonal, from_block),
            diagonal + bq // bk,
            lambda i, a: add(i, a, True),
            acc,
        )
        device = q0 // tokens
        column = pl.multiple_of(q0 % tokens, bq)
        for h in range(head_groups):
            out[device, h * width : (h + 1) * width, pl.ds(column, bq)] = acc[h].astype(bf16)
        return 0

    lax.fori_loop(0, length // bq, one_query, 0)


def final_body(returned, gates, embedded, out_weight, up, down, out):
    att = returned[...].astype(f32)
    heads = (att * rms(att, 0) * gates[...]).astype(bf16)
    hidden = embedded[...].astype(f32) + dot(heads, out_weight[...], 0, 0)
    normed = (hidden * rms(hidden, 1)).astype(bf16)
    active = silu(dot(normed, up[...], 1, 0)).astype(bf16)
    out[...] = (hidden + dot(active, down[...], 1, 0)).astype(bf16)


def local(
    token_rows,
    segment_ids,
    requests,
    hot_table,
    cold_table,
    input_weight,
    output_weight,
    up_weight,
    down_weight,
):
    both = ("emb", "seq")
    emb = lax.axis_size("emb")
    seq = lax.axis_size("seq")
    devices = emb * seq
    cap = requests.shape[2]
    hot, model = hot_table.shape
    tokens = token_rows.shape[1]
    groups = H // seq
    width = model // H
    own = lax.axis_index("seq")
    member = lax.axis_index("emb")
    span = seq * cap

    lines = tokens // LANES
    ids = token_rows.reshape(1, lines, LANES)
    below = jnp.sum(
        (segment_ids[0][None, :] < jnp.arange(SEGMENTS, dtype=jnp.int32)[:, None]).astype(
            jnp.int32
        ),
        axis=1,
    )
    edge_line = jnp.pad(below, (0, LANES - SEGMENTS)).reshape(1, 1, LANES)
    request_line = jnp.tile(requests[0], (1, LANES // cap)).reshape(devices, 1, LANES)
    message = jnp.concatenate(
        [
            jnp.broadcast_to(ids, (devices, lines, LANES)),
            request_line,
            jnp.broadcast_to(edge_line, (devices, 1, LANES)),
        ],
        axis=1,
    )
    heard = lax.all_to_all(message, both, split_axis=0, concat_axis=0, tiled=True)

    own_weight = lax.dynamic_slice_in_dim(
        input_weight, own * (groups * 4 * width), groups * 4 * width, axis=1
    )
    kept = LANES if groups == 1 else 192
    hot_projected = call(
        functools.partial(hot_body, groups),
        jax.ShapeDtypeStruct((kept, hot), bf16),
        [VMEM, VMEM],
        VMEM,
        flops=2 * hot * model * 256,
        name="hot",
    )(hot_table, own_weight)
    hot_rows = call(
        functools.partial(hot_rows_body, 512),
        jax.ShapeDtypeStruct((tokens, model), bf16),
        [VMEM, VMEM],
        VMEM,
        flops=2 * hot * model * tokens,
        name="hot_rows",
    )(token_rows.reshape(tokens, 1), hot_table)
    gate_weight = input_weight.reshape(model, H, 4, width)[:, :, 0, :].reshape(model, model)

    asked = heard[:, lines, :cap]
    sent, rows = call(
        functools.partial(owner_body, groups, emb, seq, cap),
        (
            jax.ShapeDtypeStruct(
                (devices, span if groups == 1 else span + span // 2, LANES), bf16
            ),
            jax.ShapeDtypeStruct((devices * cap, model), bf16),
        ),
        [SMEM, VMEM, ANY, VMEM],
        (VMEM, VMEM),
        [pltpu.VMEM((devices * cap * PICK, model), bf16), pltpu.SemaphoreType.DMA],
        flops=2 * devices * cap * model * 2048,
        name="owner",
    )(asked, heard, cold_table, input_weight)
    got = lax.all_to_all(sent, both, split_axis=0, concat_axis=0, tiled=True)
    fetched = lax.all_to_all(
        rows.reshape(devices, cap, model), both, split_axis=0, concat_axis=0, tiled=True
    ).reshape(devices * cap, model)

    mine = lax.dynamic_slice_in_dim(heard, member * seq, seq, axis=0)
    all_ids = mine[:, :lines].reshape(seq, tokens)
    starts = jnp.sum(mine[:, lines + 1, :SEGMENTS], axis=0)

    step = 512
    spread = pl.pallas_call(
        functools.partial(spread_body, step),
        out_shape=jax.ShapeDtypeStruct((kept, seq * tokens), bf16),
        grid=(seq,),
        in_specs=[
            pl.BlockSpec((1, 1, tokens), lambda s: (s, 0, 0)),
            pl.BlockSpec((kept, hot), lambda s: (0, 0)),
        ],
        out_specs=pl.BlockSpec((kept, tokens), lambda s: (0, s)),
        cost_estimate=pl.CostEstimate(
            flops=2 * seq * tokens * hot * 256, bytes_accessed=0, transcendentals=0
        ),
        name="spread",
    )(all_ids.reshape(seq, 1, tokens), hot_projected)

    attended = call(
        functools.partial(attend_body, groups, seq, cap, hot, width, BQ, BK),
        jax.ShapeDtypeStruct((seq, groups * width, tokens), bf16),
        [SMEM, VMEM, VMEM, VMEM],
        VMEM,
        [
            pltpu.VMEM((groups, width, seq * tokens), bf16),
            pltpu.VMEM((groups, width, seq * tokens), bf16),
            pltpu.VMEM((groups, seq * tokens, width), bf16),
        ],
        flops=10**10,
        name="attend",
    )(starts, all_ids, spread, got)
    returned = lax.all_to_all(attended, "seq", split_axis=0, concat_axis=0, tiled=True)

    embedded, gates = call(
        functools.partial(own_body, hot),
        (
            jax.ShapeDtypeStruct((tokens, model), bf16),
            jax.ShapeDtypeStruct((model, tokens), f32),
        ),
        [VMEM] * 5,
        (VMEM, VMEM),
        flops=2 * tokens * model * model,
        name="own",
    )(token_rows.reshape(tokens, 1), token_rows, hot_rows, fetched, gate_weight)
    result = call(
        final_body,
        jax.ShapeDtypeStruct((tokens, model), bf16),
        [VMEM] * 6,
        VMEM,
        flops=2 * tokens * model * 4096,
        name="final",
    )(returned.reshape(model, tokens), gates, embedded, output_weight, up_weight, down_weight)
    return result[None]


BQ = 512
BK = 256


def solution(mesh):
    placed = (
        P("emb", "seq"),
        P("emb", "seq"),
        P(("emb", "seq"), None, None),
        P(),
        P(("emb", "seq"), None),
        P(),
        P(),
        P(),
        P(),
    )
    return jax.shard_map(
        local, mesh=mesh, in_specs=placed, out_specs=P("emb", "seq", None), check_vma=False
    )
```

```python
import functools
import math

import jax
import jax.numpy as jnp
from jax import lax
from jax.experimental import pallas as pl
from jax.experimental.pallas import tpu as pltpu
from jax.sharding import PartitionSpec as P

H = 16
LANES = 128
PICK = 8
SEGMENTS = 4
epsilon = 1e-06
APART = 2.0**30
f32 = jnp.float32
bf16 = jnp.bfloat16

VMEM = pl.BlockSpec(memory_space=pltpu.VMEM)
SMEM = pl.BlockSpec(memory_space=pltpu.SMEM)
HBM = pl.BlockSpec(memory_space=pl.ANY)


def call(body, out_shape, in_specs, out_specs, scratch=(), flops=0, name=None, size=60):
    return pl.pallas_call(
        body,
        out_shape=out_shape,
        in_specs=in_specs,
        out_specs=out_specs,
        scratch_shapes=list(scratch),
        compiler_params=pltpu.CompilerParams(vmem_limit_bytes=size * 1024 * 1024),
        cost_estimate=pl.CostEstimate(flops=flops, bytes_accessed=0, transcendentals=0),
        name=name,
    )


def dot(a, b, ca, cb):
    return lax.dot_general(a, b, (((ca,), (cb,)), ((), ())), preferred_element_type=f32)


def silu(x):
    half = x * 0.5
    return half * jnp.tanh(half) + half


def rms(x, axis):
    return lax.rsqrt(jnp.mean(x * x, axis=axis, keepdims=True) + epsilon)


def owner_body(
    head_groups, emb, seq, cap, message_hbm, message, cold, weight_hbm, after,
    sent, tiles, weight, req, sem, weight_sem,
):
    count = emb * seq * cap
    per = LANES // cap
    span = seq * cap
    split = weight.shape[0] // LANES
    raw = cap * split
    load = pltpu.make_async_copy(weight_hbm, weight, weight_sem)

    asked = pltpu.make_async_copy(message_hbm.at[:, message.shape[1] - 2, :], req, weight_sem)
    asked.start()
    asked.wait()
    batch = 8

    def fetch(j, _):
        for i in range(batch):
            for k in range(cap):
                row = req[j * batch + i, k]
                base = pl.multiple_of((row // PICK) * PICK, PICK)
                slot = pl.multiple_of(((j * batch + i) * cap + k) * PICK, PICK)
                pltpu.make_async_copy(
                    cold.at[pl.ds(base, PICK)], tiles.at[pl.ds(slot, PICK)], sem
                ).start()
        return 0

    lax.fori_loop(0, emb * seq // batch, fetch, 0)
    load.start()
    tags = message[:, message.shape[1] - 2, :]
    picks = []
    for group in range(count // LANES):
        owner = lax.broadcasted_iota(jnp.int32, (per, LANES), 0)
        lane = lax.broadcasted_iota(jnp.int32, (per, LANES), 1)
        mine = jnp.where(lane // cap == owner, tags[group * per : (group + 1) * per], 0)
        wanted = jnp.sum(mine, axis=0, keepdims=True)
        place = lax.broadcasted_iota(jnp.int32, (LANES * PICK, LANES), 0)
        column = lax.broadcasted_iota(jnp.int32, (1, LANES), 1)
        pick = (place == column * PICK + wanted % PICK).astype(f32)
        picks.append(pick.T.astype(bf16))
    line = lax.broadcasted_iota(jnp.int32, (per * raw, LANES), 0)
    source = lax.broadcasted_iota(jnp.int32, (per * raw, LANES), 1)
    repeat = ((line // raw) * cap + line % cap == source).astype(f32).astype(bf16)
    chunk = (lax.broadcasted_iota(jnp.int32, (per * raw, LANES), 0) % raw) // cap
    pltpu.make_async_copy(cold.at[pl.ds(0, count * PICK)], tiles, sem).wait()
    load.wait()
    for group in range(count // LANES):
        block = tiles[group * LANES * PICK : (group + 1) * LANES * PICK]
        part = dot(picks[group], block, 1, 0)
        normed = (part * rms(part, 1)).astype(bf16)
        projected = dot(normed, weight[...], 1, 0).astype(bf16)
        spread = dot(repeat, part.astype(bf16), 1, 0)
        lines = spread[:, :LANES]
        for c in range(1, split):
            lines = jnp.where(chunk == c, spread[:, c * LANES : (c + 1) * LANES], lines)
        kept = sent.shape[1] - raw
        sent[group * per : (group + 1) * per, kept:] = lines.astype(bf16).reshape(
            per, raw, LANES
        )
        for local in range(LANES // span):
            member = group * (LANES // span) + local
            for g in range(seq):
                piece = projected[local * span : (local + 1) * span]
                if head_groups == 1:
                    sent[member * seq + g, :span] = piece[:, g * LANES : (g + 1) * LANES]
                else:
                    low = piece[:, (2 * g) * LANES : (2 * g + 1) * LANES]
                    high = piece[:, (2 * g + 1) * LANES : (2 * g + 2) * LANES]
                    sent[member * seq + g, :span] = jnp.concatenate(
                        [high[:, 32:64], low[:, 32:]], axis=1
                    )
                    sent[member * seq + g, span:kept] = jnp.concatenate(
                        [high[span // 2 :, 64:], high[: span // 2, 64:]], axis=1
                    )


def message_body(ids, segments, wanted, out):
    devices, lines, _ = out.shape
    cap = wanted.shape[0]
    lane = lax.broadcasted_iota(jnp.int32, (1, LANES), 1)
    edges = jnp.zeros((1, LANES), jnp.int32)
    for s in range(1, SEGMENTS):
        below = jnp.sum((segments[...] < s).astype(jnp.int32), axis=1, keepdims=True)
        edges = jnp.where(lane == s, below, edges)
    for j in range(lines - 2):
        out[:, j, :] = jnp.broadcast_to(
            ids[:, j * LANES : (j + 1) * LANES], (devices, LANES)
        )
    asked = wanted[...].astype(f32).T.astype(jnp.int32)
    tags = jnp.broadcast_to(asked[:, 0:1], (devices, LANES))
    for k in range(1, cap):
        tags = jnp.where(lane % cap == k, asked[:, k : k + 1], tags)
    out[:, lines - 2, :] = tags
    out[:, lines - 1, :] = jnp.broadcast_to(edges, (devices, LANES))


def hot_body(head_groups, step, own, after, weight_hbm, table_hbm, out_hbm, weight, table, out, sems):
    hot = table.shape[0]
    chunks = hot // step
    lanes = weight.shape[1]
    begin = pl.multiple_of(own[0] * lanes, lanes)
    first = pltpu.make_async_copy(
        weight_hbm.at[:, pl.ds(begin, lanes)], weight, sems.at[2 * chunks]
    )
    first.start()
    loads = [
        pltpu.make_async_copy(
            table_hbm.at[pl.ds(c * step, step)], table.at[pl.ds(c * step, step)], sems.at[c]
        )
        for c in range(chunks)
    ]
    saves = [
        pltpu.make_async_copy(
            out.at[:, pl.ds(c * step, step)],
            out_hbm.at[:, pl.ds(c * step, step)],
            sems.at[chunks + c],
        )
        for c in range(chunks)
    ]
    for load in loads:
        load.start()
    first.wait()
    wide = weight[...].astype(f32).T.astype(bf16)
    for c in range(chunks):
        at = slice(c * step, (c + 1) * step)
        loads[c].wait()
        x = table[at].astype(f32)
        normed = (x * rms(x, 1)).astype(bf16)
        flat = dot(wide, normed, 1, 1).astype(bf16)
        if head_groups == 1:
            out[:, at] = flat
        else:
            out[0:32, at] = flat[160:192]
            out[32:128, at] = flat[32:128]
            out[128:192, at] = flat[192:256]
        saves[c].start()
    for save in saves:
        save.wait()


def item_row(heard, at, lines):
    return jnp.concatenate([heard[at, j : j + 1, :] for j in range(lines)], axis=1)


def spread_body(step, seq, lines, member, heard, table_hbm, out_hbm, base, table, out, sems):
    tokens = lines * LANES
    hot = table.shape[1]
    load = pltpu.make_async_copy(table_hbm, table, sems.at[seq])
    load.start()
    base[...] = lax.broadcasted_iota(jnp.int32, base.shape, 0).astype(jnp.int16)
    load.wait()

    def save(s):
        column = pl.multiple_of(s * tokens, tokens)
        return pltpu.make_async_copy(
            out.at[:, pl.ds(column, tokens)], out_hbm.at[:, pl.ds(column, tokens)], sems.at[s]
        )

    def one(s, _):
        own = item_row(heard, member[0] * seq + s, lines)
        column = pl.multiple_of(s * tokens, tokens)
        acc = jnp.zeros((out.shape[0], tokens), f32)
        for c in range(hot // step):
            place = (own - c * step).astype(jnp.int16)
            pick = jnp.where(base[...] == place, jnp.ones((), bf16), jnp.zeros((), bf16))
            acc = acc + dot(table[:, c * step : (c + 1) * step], pick, 1, 0)
        out[:, pl.ds(column, tokens)] = acc.astype(bf16)
        save(s).start()
        return 0

    lax.fori_loop(0, seq, one, 0)
    for s in range(seq):
        save(s).wait()


def own_body(
    hot, cap, step, ids, got, table_hbm, weight_hbm, embedded_hbm, gates_hbm,
    table, weight, embedded, gates, sems,
):
    tokens, model = embedded.shape
    chunks = hot // step
    loads = [
        pltpu.make_async_copy(
            table_hbm.at[pl.ds(c * step, step)], table.at[pl.ds(c * step, step)], sems.at[3 + c]
        )
        for c in range(chunks)
    ]
    for load in loads:
        load.start()
    load = pltpu.make_async_copy(weight_hbm, weight, sems.at[0])
    load.start()
    items = jnp.broadcast_to(ids[...].astype(f32), (8, tokens)).T[:, 0:1].astype(jnp.int32)
    split = model // LANES
    raw = cap * split
    owners = got.shape[0]
    lines = got[:, got.shape[1] - raw :, :].reshape(owners * raw, LANES)
    slot = items - hot
    code = jnp.where(slot >= 0, (slot // cap) * raw + slot % cap, -raw)
    place = lax.broadcasted_iota(jnp.int32, (tokens, owners * raw), 1)
    parts = []
    for c in range(split):
        pick = (place == code + c * cap).astype(f32).astype(bf16)
        parts.append(dot(pick, lines, 1, 0))
    emb = jnp.concatenate(parts, axis=1)
    for c in range(chunks):
        loads[c].wait()
        place = lax.broadcasted_iota(jnp.int32, (tokens, step), 1) + c * step
        pick = (place == items).astype(f32).astype(bf16)
        emb = emb + dot(pick, table[c * step : (c + 1) * step], 1, 0)
    embedded[...] = emb.astype(bf16)
    save = pltpu.make_async_copy(embedded, embedded_hbm, sems.at[1])
    save.start()
    normed = (emb * rms(emb, 1)).astype(bf16)
    load.wait()
    step = weight.shape[1] // H
    width = model // H
    wide = jnp.concatenate(
        [
            weight[:, h * step : (h + 1) * step].astype(f32).T[:width]
            for h in range(H)
        ],
        axis=0,
    ).astype(bf16)
    u = dot(wide, normed, 1, 1).astype(bf16).astype(f32)
    gates[...] = silu(u)
    other = pltpu.make_async_copy(gates, gates_hbm, sems.at[2])
    other.start()
    save.wait()
    other.wait()


def attend_body(
    head_groups, seq, cap, hot, width, bq, bk, lines, member, heard, table_hbm, got, out,
    qt, vt, kr, score0, score1, weight0, weight1, total, table, base, sems
):
    tokens = lines * LANES
    length = seq * tokens
    owners = got.shape[0]
    quarter = 16 // cap
    span = seq * cap
    depth = qt.shape[1]
    kept = span if head_groups == 1 else span + span // 2
    loads = [
        pltpu.make_async_copy(
            table_hbm.at[:, pl.ds(s * tokens, tokens)],
            table.at[:, pl.ds(s * tokens, tokens)],
            sems.at[s],
        )
        for s in range(seq)
    ]
    for load in loads:
        load.start()
    mine = heard[pl.ds(member[0] * seq, seq), lines + 1, :]
    lane = lax.broadcasted_iota(jnp.int32, mine.shape, 1)
    edges = [jnp.sum(jnp.where(lane == i, mine, 0)) for i in range(1, SEGMENTS)]
    base[...] = lax.broadcasted_iota(jnp.int32, base.shape, 0).astype(jnp.int16)
    for part in range(span // 16):
        a = got[:, part * 16 : (part + 1) * 16, :].reshape(owners * 16, LANES)
        if head_groups == 1:
            lhs = a.astype(f32).T.astype(bf16)
        else:
            b = got[:, span:kept, :].reshape(owners * 16, LANES).astype(f32).T
            b = b[64:] if part == 0 else b[:64]
            lhs = jnp.concatenate([a.astype(f32).T, b], axis=0).astype(bf16)
        for within in range(quarter):
            s = part * quarter + within
            slot = item_row(heard, member[0] * seq + s, lines) - hot
            code = jnp.where(slot >= 0, (slot // cap) * 16 + within * cap + slot % cap, -1)
            pick = jnp.where(
                base[...] == code.astype(jnp.int16), jnp.ones((), bf16), jnp.zeros((), bf16)
            )
            at = slice(s * tokens, (s + 1) * tokens)
            loads[s].wait()
            full = dot(lhs, pick, 1, 0) + table[:, at].astype(f32)
            full_b = full.astype(bf16)
            spot = s * tokens + lax.broadcasted_iota(jnp.int32, (1, tokens), 1)
            segment = jnp.zeros((1, tokens), jnp.int32)
            for edge in edges:
                segment = segment + (spot >= edge).astype(jnp.int32)
            level = lax.broadcasted_iota(jnp.int32, (depth - width, tokens), 0)
            same = (level == segment).astype(f32)
            if head_groups == 1:
                order = ((32, 64, 96),)
            else:
                order = ((32, 64, 96), (0, 128, 160))
            for h, (v, q, k) in enumerate(order):
                vt[h, :, at] = full_b[v : v + width]
                qt[h, :, at] = jnp.concatenate(
                    [full_b[q : q + width], ((same - 1.0) * APART).astype(bf16)], axis=0
                )
                kr[h, at, :] = jnp.concatenate([full[k : k + width], same], axis=0).T.astype(
                    bf16
                )
    scale = 0.5 / math.sqrt(width)
    blocks = length // bq

    def low(qb):
        best = 0
        for edge in edges:
            best = jnp.where(qb * bq >= edge, edge, best)
        return best // bk

    def high(qb):
        return (qb + 1) * (bq // bk) - 1

    def count(qb, n):
        return n + high(qb) - low(qb) + 1

    tiles = lax.fori_loop(0, blocks, count, 0)

    ahead = lax.broadcasted_iota(jnp.int32, (bk, bq), 0) - lax.broadcasted_iota(
        jnp.int32, (bk, bq), 1
    )
    score = (score0, score1)
    weights = (weight0, weight1)

    def half_step(i, slot, now, then, past):
        qb, kb = then
        keep = ahead <= qb * bq - kb * bk
        for h in range(head_groups):
            half = score[1 - slot][h] * scale
            weight = half * jnp.tanh(half) + half
            weights[1 - slot][h] = jnp.where(keep, weight, 0.0).astype(bf16)
        qb, kb = past
        q0 = pl.multiple_of(qb * bq, bq)
        k0 = pl.multiple_of(kb * bk, bk)
        device = q0 // tokens
        column = pl.multiple_of(q0 % tokens, bq)
        fresh = kb == low(qb)
        live = (i >= 2) & (i < tiles + 2)
        for h in range(head_groups):
            part = dot(vt[h, :, pl.ds(k0, bk)], weights[slot][h], 1, 0)
            part = jnp.where(live, part + jnp.where(fresh, 0.0, total[h]), total[h])
            total[h] = part
            out[device, h * width : (h + 1) * width, pl.ds(column, bq)] = part.astype(bf16)
        qb, kb = now
        q0 = pl.multiple_of(qb * bq, bq)
        k0 = pl.multiple_of(kb * bk, bk)
        for h in range(head_groups):
            score[slot][h] = dot(kr[h, pl.ds(k0, bk), :], qt[h, :, pl.ds(q0, bq)], 1, 0)
        done = kb == high(qb)
        last = done & (qb == blocks - 1)
        next_q = jnp.where(done & ~last, qb + 1, qb)
        next_k = jnp.where(last, kb, jnp.where(done, low(next_q), kb + 1))
        return next_q, next_k

    def step(j, state):
        now, then, past = state
        after = half_step(2 * j, 0, now, then, past)
        later = half_step(2 * j + 1, 1, after, now, then)
        return later, after, now

    start = (jnp.int32(0), jnp.int32(0))
    for ref in (score1, weight0):
        ref[...] = jnp.zeros(ref.shape, ref.dtype)
    total[...] = jnp.zeros(total.shape, f32)
    lax.fori_loop(0, (tiles + 3) // 2, step, (start, start, start))


def final_body(
    returned, gates_hbm, embedded_hbm, out_hbm, up_hbm, down_hbm, result,
    gates, embedded, out_weight, up, down, out, sems,
):
    tokens = out.shape[0]
    pairs = (
        (gates_hbm, gates),
        (out_hbm, out_weight),
        (embedded_hbm, embedded),
        (up_hbm, up),
        (down_hbm, down),
    )
    loads = [
        pltpu.make_async_copy(there, here, sems.at[i]) for i, (there, here) in enumerate(pairs)
    ]
    for load in loads:
        load.start()
    att = returned[...].astype(f32)
    att = att * rms(att, 0)
    loads[0].wait()
    heads = (att * gates[...]).astype(bf16)
    loads[1].wait()
    mixed = dot(heads, out_weight[...], 0, 0)
    loads[2].wait()
    hidden = embedded[...].astype(f32) + mixed
    normed = (hidden * rms(hidden, 1)).astype(bf16)
    loads[3].wait()
    saves = []
    half = tokens // 2
    for part in range(2):
        at = slice(part * half, (part + 1) * half)
        active = silu(dot(normed[at], up[...], 1, 0)).astype(bf16)
        if part == 0:
            loads[4].wait()
        out[at] = (hidden[at] + dot(active, down[...], 1, 0)).astype(bf16)
        saves.append(
            pltpu.make_async_copy(
                out.at[pl.ds(part * half, half)],
                result.at[pl.ds(part * half, half)],
                sems.at[5 + part],
            )
        )
        saves[-1].start()
    for save in saves:
        save.wait()


def local(
    token_rows,
    segment_ids,
    requests,
    hot_table,
    cold_table,
    input_weight,
    output_weight,
    up_weight,
    down_weight,
):
    both = ("emb", "seq")
    emb = lax.axis_size("emb")
    seq = lax.axis_size("seq")
    devices = emb * seq
    cap = requests.shape[2]
    hot, model = hot_table.shape
    tokens = token_rows.shape[1]
    groups = H // seq
    width = model // H
    own = lax.axis_index("seq")
    member = lax.axis_index("emb")
    span = seq * cap

    lines = tokens // LANES
    raw = cap * model // LANES
    message = call(
        message_body,
        jax.ShapeDtypeStruct((devices, lines + 2, LANES), jnp.int32),
        [VMEM] * 3,
        VMEM,
        name="message",
        size=60,
    )(token_rows, segment_ids, requests[0].T)
    heard = lax.all_to_all(message, both, split_axis=0, concat_axis=0, tiled=True)

    kept = LANES if groups == 1 else 192
    step = 512
    hot_projected = call(
        functools.partial(hot_body, groups, step),
        jax.ShapeDtypeStruct((kept, hot), bf16),
        [SMEM, HBM, HBM, HBM],
        HBM,
        [
            pltpu.VMEM((model, groups * 4 * width), bf16),
            pltpu.VMEM((hot, model), bf16),
            pltpu.VMEM((kept, hot), bf16),
            pltpu.SemaphoreType.DMA((2 * (hot // step) + 1,)),
        ],
        flops=2 * hot * model * 256,
        name="hot",
        size=60,
    )(own.astype(jnp.int32).reshape(1), message, input_weight, hot_table)

    span_lines = span if groups == 1 else span + span // 2
    sent = call(
        functools.partial(owner_body, groups, emb, seq, cap),
        jax.ShapeDtypeStruct((devices, span_lines + raw, LANES), bf16),
        [HBM, VMEM, HBM, HBM, HBM],
        VMEM,
        [
            pltpu.VMEM((devices * cap * PICK, model), bf16),
            pltpu.VMEM(input_weight.shape, bf16),
            pltpu.SMEM((devices, LANES), jnp.int32),
            pltpu.SemaphoreType.DMA,
            pltpu.SemaphoreType.DMA,
        ],
        flops=2 * devices * cap * model * 2048,
        name="owner",
        size=60,
    )(heard, heard, cold_table, input_weight, hot_projected)
    got = lax.all_to_all(sent, both, split_axis=0, concat_axis=0, tiled=True)

    place = member.astype(jnp.int32).reshape(1)
    spread = call(
        functools.partial(spread_body, step, seq, lines),
        jax.ShapeDtypeStruct((kept, seq * tokens), bf16),
        [SMEM, VMEM, HBM],
        HBM,
        [
            pltpu.VMEM((step, tokens), jnp.int16),
            pltpu.VMEM((kept, hot), bf16),
            pltpu.VMEM((kept, seq * tokens), bf16),
            pltpu.SemaphoreType.DMA((seq + 1,)),
        ],
        flops=2 * seq * tokens * hot * 256,
        name="spread",
        size=60,
    )(place, heard, hot_projected)

    deep = width + 16
    tile = (groups, BK, BQ)
    attended = call(
        functools.partial(attend_body, groups, seq, cap, hot, width, BQ, BK, lines),
        jax.ShapeDtypeStruct((seq, groups * width, tokens), bf16),
        [SMEM, VMEM, HBM, VMEM],
        VMEM,
        [
            pltpu.VMEM((groups, deep, seq * tokens), bf16),
            pltpu.VMEM((groups, width, seq * tokens), bf16),
            pltpu.VMEM((groups, seq * tokens, deep), bf16),
            pltpu.VMEM(tile, f32),
            pltpu.VMEM(tile, f32),
            pltpu.VMEM(tile, bf16),
            pltpu.VMEM(tile, bf16),
            pltpu.VMEM((groups, width, BQ), f32),
            pltpu.VMEM((kept, seq * tokens), bf16),
            pltpu.VMEM((devices * 16, tokens), jnp.int16),
            pltpu.SemaphoreType.DMA((seq,)),
        ],
        flops=10**10,
        name="attend",
        size=60,
    )(place, heard, spread, got)
    returned = lax.all_to_all(attended, "seq", split_axis=0, concat_axis=0, tiled=True)

    embedded, gates = call(
        functools.partial(own_body, hot, cap, step),
        (
            jax.ShapeDtypeStruct((tokens, model), bf16),
            jax.ShapeDtypeStruct((model, tokens), f32),
        ),
        [VMEM, VMEM, HBM, HBM],
        (HBM, HBM),
        [
            pltpu.VMEM((hot, model), bf16),
            pltpu.VMEM(input_weight.shape, bf16),
            pltpu.VMEM((tokens, model), bf16),
            pltpu.VMEM((model, tokens), f32),
            pltpu.SemaphoreType.DMA((3 + hot // step,)),
        ],
        flops=2 * tokens * model * model,
        name="own",
        size=60,
    )(token_rows, got, hot_table, input_weight)
    result = call(
        final_body,
        jax.ShapeDtypeStruct((tokens, model), bf16),
        [VMEM, HBM, HBM, HBM, HBM, HBM],
        HBM,
        [
            pltpu.VMEM((model, tokens), f32),
            pltpu.VMEM((tokens, model), bf16),
            pltpu.VMEM(output_weight.shape, bf16),
            pltpu.VMEM(up_weight.shape, bf16),
            pltpu.VMEM(down_weight.shape, bf16),
            pltpu.VMEM((tokens, model), bf16),
            pltpu.SemaphoreType.DMA((7,)),
        ],
        flops=2 * tokens * model * 4096,
        name="final",
        size=60,
    )(returned.reshape(model, tokens), gates, embedded, output_weight, up_weight, down_weight)
    return result[None]


BQ = 256
BK = 256


def solution(mesh):
    placed = (
        P("emb", "seq"),
        P("emb", "seq"),
        P(("emb", "seq"), None, None),
        P(),
        P(("emb", "seq"), None),
        P(),
        P(),
        P(),
        P(),
    )
    return jax.shard_map(
        local, mesh=mesh, in_specs=placed, out_specs=P("emb", "seq", None), check_vma=False
    )
```

```python
import functools
import math

import jax
import jax.numpy as jnp
from jax import lax
from jax.experimental import pallas as pl
from jax.experimental.pallas import tpu as pltpu
from jax.sharding import PartitionSpec as P

H = 16
LANES = 128
PICK = 8
SEGMENTS = 4
epsilon = 1e-06
APART = 2.0**30
f32 = jnp.float32
bf16 = jnp.bfloat16

VMEM = pl.BlockSpec(memory_space=pltpu.VMEM)
SMEM = pl.BlockSpec(memory_space=pltpu.SMEM)
HBM = pl.BlockSpec(memory_space=pl.ANY)


def call(body, out_shape, in_specs, out_specs, scratch=(), flops=0, name=None, size=60):
    return pl.pallas_call(
        body,
        out_shape=out_shape,
        in_specs=in_specs,
        out_specs=out_specs,
        scratch_shapes=list(scratch),
        compiler_params=pltpu.CompilerParams(vmem_limit_bytes=size * 1024 * 1024),
        cost_estimate=pl.CostEstimate(flops=flops, bytes_accessed=0, transcendentals=0),
        name=name,
    )


def dot(a, b, ca, cb):
    return lax.dot_general(a, b, (((ca,), (cb,)), ((), ())), preferred_element_type=f32)


def silu(x):
    half = x * 0.5
    return half * jnp.tanh(half) + half


def rms(x, axis):
    return lax.rsqrt(jnp.mean(x * x, axis=axis, keepdims=True) + epsilon)


def owner_body(
    head_groups, emb, seq, cap, message_hbm, cold, weight_hbm, after, sent_hbm,
    sent, tiles, weight, req, tags, sem, weight_sem, sems,
):
    count = emb * seq * cap
    per = LANES // cap
    span = seq * cap
    split = weight.shape[0] // LANES
    raw = cap * split
    load = pltpu.make_async_copy(weight_hbm, weight, weight_sem)

    wanted_line = message_hbm.shape[1] - 2
    asked = pltpu.make_async_copy(message_hbm.at[:, wanted_line, :], req, sems.at[0])
    asked.start()
    again = pltpu.make_async_copy(message_hbm.at[:, wanted_line, :], tags, sems.at[1])
    again.start()
    load.start()
    asked.wait()
    batch = 8

    def fetch(j, _):
        for i in range(batch):
            for k in range(cap):
                row = req[j * batch + i, k]
                base = pl.multiple_of((row // PICK) * PICK, PICK)
                slot = pl.multiple_of(((j * batch + i) * cap + k) * PICK, PICK)
                pltpu.make_async_copy(
                    cold.at[pl.ds(base, PICK)], tiles.at[pl.ds(slot, PICK)], sem
                ).start()
        return 0

    lax.fori_loop(0, emb * seq // batch, fetch, 0)
    again.wait()
    picks = []
    for group in range(count // LANES):
        owner = lax.broadcasted_iota(jnp.int32, (per, LANES), 0)
        lane = lax.broadcasted_iota(jnp.int32, (per, LANES), 1)
        mine = jnp.where(lane // cap == owner, tags[group * per : (group + 1) * per], 0)
        wanted = jnp.sum(mine, axis=0, keepdims=True)
        place = lax.broadcasted_iota(jnp.int32, (LANES * PICK, LANES), 0)
        column = lax.broadcasted_iota(jnp.int32, (1, LANES), 1)
        pick = (place == column * PICK + wanted % PICK).astype(f32)
        picks.append(pick.T.astype(bf16))
    line = lax.broadcasted_iota(jnp.int32, (per * raw, LANES), 0)
    source = lax.broadcasted_iota(jnp.int32, (per * raw, LANES), 1)
    repeat = ((line // raw) * cap + line % cap == source).astype(f32).astype(bf16)
    chunk = (lax.broadcasted_iota(jnp.int32, (per * raw, LANES), 0) % raw) // cap
    saves = []
    pltpu.make_async_copy(cold.at[pl.ds(0, count * PICK)], tiles, sem).wait()
    load.wait()
    for group in range(count // LANES):
        block = tiles[group * LANES * PICK : (group + 1) * LANES * PICK]
        part = dot(picks[group], block, 1, 0)
        normed = (part * rms(part, 1)).astype(bf16)
        projected = dot(normed, weight[...], 1, 0).astype(bf16)
        spread = dot(repeat, part.astype(bf16), 1, 0)
        lines = spread[:, :LANES]
        for c in range(1, split):
            lines = jnp.where(chunk == c, spread[:, c * LANES : (c + 1) * LANES], lines)
        kept = sent.shape[1] - raw
        sent[group * per : (group + 1) * per, kept:] = lines.astype(bf16).reshape(
            per, raw, LANES
        )
        for local in range(LANES // span):
            member = group * (LANES // span) + local
            for g in range(seq):
                piece = projected[local * span : (local + 1) * span]
                if head_groups == 1:
                    sent[member * seq + g, :span] = piece[:, g * LANES : (g + 1) * LANES]
                else:
                    low = piece[:, (2 * g) * LANES : (2 * g + 1) * LANES]
                    high = piece[:, (2 * g + 1) * LANES : (2 * g + 2) * LANES]
                    sent[member * seq + g, :span] = jnp.concatenate(
                        [high[:, 32:64], low[:, 32:]], axis=1
                    )
                    sent[member * seq + g, span:kept] = jnp.concatenate(
                        [high[span // 2 :, 64:], high[: span // 2, 64:]], axis=1
                    )
            at = pl.ds(member * seq, seq)
            saves.append(
                pltpu.make_async_copy(sent.at[at], sent_hbm.at[at], sems.at[2 + len(saves)])
            )
            saves[-1].start()
    for save in saves:
        save.wait()


def message_body(ids, segments, wanted, out):
    devices, lines, _ = out.shape
    cap = wanted.shape[0]
    lane = lax.broadcasted_iota(jnp.int32, (1, LANES), 1)
    edges = jnp.zeros((1, LANES), jnp.int32)
    for s in range(1, SEGMENTS):
        below = jnp.sum((segments[...] < s).astype(jnp.int32), axis=1, keepdims=True)
        edges = jnp.where(lane == s, below, edges)
    for j in range(lines - 2):
        out[:, j, :] = jnp.broadcast_to(
            ids[:, j * LANES : (j + 1) * LANES], (devices, LANES)
        )
    asked = wanted[...].astype(f32).T.astype(jnp.int32)
    tags = jnp.broadcast_to(asked[:, 0:1], (devices, LANES))
    for k in range(1, cap):
        tags = jnp.where(lane % cap == k, asked[:, k : k + 1], tags)
    out[:, lines - 2, :] = tags
    out[:, lines - 1, :] = jnp.broadcast_to(edges, (devices, LANES))


def hot_body(head_groups, step, own, after, weight_hbm, table_hbm, out_hbm, weight, table, out, sems):
    hot = table.shape[0]
    chunks = hot // step
    lanes = weight.shape[1]
    begin = pl.multiple_of(own[0] * lanes, lanes)
    first = pltpu.make_async_copy(
        weight_hbm.at[:, pl.ds(begin, lanes)], weight, sems.at[2 * chunks]
    )
    first.start()
    loads = [
        pltpu.make_async_copy(
            table_hbm.at[pl.ds(c * step, step)], table.at[pl.ds(c * step, step)], sems.at[c]
        )
        for c in range(chunks)
    ]
    saves = [
        pltpu.make_async_copy(
            out.at[:, pl.ds(c * step, step)],
            out_hbm.at[:, pl.ds(c * step, step)],
            sems.at[chunks + c],
        )
        for c in range(chunks)
    ]
    for load in loads:
        load.start()
    first.wait()
    wide = weight[...].astype(f32).T.astype(bf16)
    for c in range(chunks):
        at = slice(c * step, (c + 1) * step)
        loads[c].wait()
        x = table[at].astype(f32)
        normed = (x * rms(x, 1)).astype(bf16)
        flat = dot(wide, normed, 1, 1).astype(bf16)
        if head_groups == 1:
            out[:, at] = flat
        else:
            out[0:32, at] = flat[160:192]
            out[32:128, at] = flat[32:128]
            out[128:192, at] = flat[192:256]
        saves[c].start()
    for save in saves:
        save.wait()


def item_row(heard, at, lines):
    return jnp.concatenate([heard[at, j : j + 1, :] for j in range(lines)], axis=1)


def spread_body(step, seq, lines, member, heard, table_hbm, out_hbm, base, table, out, sems):
    tokens = lines * LANES
    hot = table.shape[1]
    load = pltpu.make_async_copy(table_hbm, table, sems.at[seq])
    load.start()
    base[...] = lax.broadcasted_iota(jnp.int32, base.shape, 0).astype(jnp.int16)
    load.wait()

    def save(s):
        column = pl.multiple_of(s * tokens, tokens)
        return pltpu.make_async_copy(
            out.at[:, pl.ds(column, tokens)], out_hbm.at[:, pl.ds(column, tokens)], sems.at[s]
        )

    def one(s, _):
        own = item_row(heard, member[0] * seq + s, lines)
        column = pl.multiple_of(s * tokens, tokens)
        acc = jnp.zeros((out.shape[0], tokens), f32)
        for c in range(hot // step):
            place = (own - c * step).astype(jnp.int16)
            pick = jnp.where(base[...] == place, jnp.ones((), bf16), jnp.zeros((), bf16))
            acc = acc + dot(table[:, c * step : (c + 1) * step], pick, 1, 0)
        out[:, pl.ds(column, tokens)] = acc.astype(bf16)
        save(s).start()
        return 0

    lax.fori_loop(0, seq, one, 0)
    for s in range(seq):
        save(s).wait()


def own_body(
    hot, cap, step, ids, got, table_hbm, weight_hbm, out_hbm, carried,
    table, weight, embedded, gates, out_weight, sems,
):
    tokens, model = embedded.shape
    chunks = hot // step
    loads = [
        pltpu.make_async_copy(
            table_hbm.at[pl.ds(c * step, step)], table.at[pl.ds(c * step, step)], sems.at[3 + c]
        )
        for c in range(chunks)
    ]
    for load in loads:
        load.start()
    load = pltpu.make_async_copy(weight_hbm, weight, sems.at[0])
    load.start()
    third = pltpu.make_async_copy(out_hbm, out_weight, sems.at[3 + chunks])
    third.start()
    items = jnp.broadcast_to(ids[...].astype(f32), (8, tokens)).T[:, 0:1].astype(jnp.int32)
    split = model // LANES
    raw = cap * split
    owners = got.shape[0]
    lines = got[:, got.shape[1] - raw :, :].reshape(owners * raw, LANES)
    slot = items - hot
    code = jnp.where(slot >= 0, (slot // cap) * raw + slot % cap, -raw)
    place = lax.broadcasted_iota(jnp.int32, (tokens, owners * raw), 1)
    parts = []
    for c in range(split):
        pick = (place == code + c * cap).astype(f32).astype(bf16)
        parts.append(dot(pick, lines, 1, 0))
    emb = jnp.concatenate(parts, axis=1)
    for c in range(chunks):
        loads[c].wait()
        place = lax.broadcasted_iota(jnp.int32, (tokens, step), 1) + c * step
        pick = (place == items).astype(f32).astype(bf16)
        emb = emb + dot(pick, table[c * step : (c + 1) * step], 1, 0)
    embedded[...] = emb.astype(bf16)
    save = pltpu.make_async_copy(embedded, carried.at[pl.ds(model, tokens)], sems.at[1])
    save.start()
    third.wait()
    third = pltpu.make_async_copy(
        out_weight, carried.at[pl.ds(model + tokens, model)], sems.at[3 + chunks]
    )
    third.start()
    normed = (emb * rms(emb, 1)).astype(bf16)
    load.wait()
    step = weight.shape[1] // H
    width = model // H
    wide = jnp.concatenate(
        [
            weight[:, h * step : (h + 1) * step].astype(f32).T[:width]
            for h in range(H)
        ],
        axis=0,
    ).astype(bf16)
    u = dot(wide, normed, 1, 1).astype(bf16).astype(f32)
    gates[...] = silu(u).astype(bf16)
    other = pltpu.make_async_copy(gates, carried.at[pl.ds(0, model)], sems.at[2])
    other.start()
    save.wait()
    third.wait()
    other.wait()


def attend_body(
    head_groups, seq, cap, hot, width, bq, bk, lines, member, heard, table_hbm, got, out,
    qt, vt, kr, score0, score1, weight0, weight1, total, table, base, factor, sems
):
    tokens = lines * LANES
    length = seq * tokens
    owners = got.shape[0]
    quarter = 16 // cap
    span = seq * cap
    depth = qt.shape[1]
    kept = span if head_groups == 1 else span + span // 2
    loads = [
        pltpu.make_async_copy(
            table_hbm.at[:, pl.ds(s * tokens, tokens)],
            table.at[:, pl.ds(s * tokens, tokens)],
            sems.at[s],
        )
        for s in range(seq)
    ]
    for load in loads:
        load.start()
    mine = heard[pl.ds(member[0] * seq, seq), lines + 1, :]
    lane = lax.broadcasted_iota(jnp.int32, mine.shape, 1)
    edges = [jnp.sum(jnp.where(lane == i, mine, 0)) for i in range(1, SEGMENTS)]
    base[...] = lax.broadcasted_iota(jnp.int32, base.shape, 0).astype(jnp.int16)
    for part in range(span // 16):
        a = got[:, part * 16 : (part + 1) * 16, :].reshape(owners * 16, LANES)
        if head_groups == 1:
            lhs = a.astype(f32).T.astype(bf16)
        else:
            b = got[:, span:kept, :].reshape(owners * 16, LANES).astype(f32).T
            b = b[64:] if part == 0 else b[:64]
            lhs = jnp.concatenate([a.astype(f32).T, b], axis=0).astype(bf16)
        for within in range(quarter):
            s = part * quarter + within
            slot = item_row(heard, member[0] * seq + s, lines) - hot
            code = jnp.where(slot >= 0, (slot // cap) * 16 + within * cap + slot % cap, -1)
            pick = jnp.where(
                base[...] == code.astype(jnp.int16), jnp.ones((), bf16), jnp.zeros((), bf16)
            )
            at = slice(s * tokens, (s + 1) * tokens)
            loads[s].wait()
            full = dot(lhs, pick, 1, 0).astype(bf16) + table[:, at]
            spot = s * tokens + lax.broadcasted_iota(jnp.int32, (1, tokens), 1)
            segment = jnp.zeros((1, tokens), jnp.int32)
            for edge in edges:
                segment = segment + (spot >= edge).astype(jnp.int32)
            level = lax.broadcasted_iota(jnp.int32, (depth - width, tokens), 0)
            same = (level == segment).astype(f32)
            apart = ((same - 1.0) * APART).astype(bf16)
            same = same.astype(bf16)
            if head_groups == 1:
                order = ((32, 64, 96),)
            else:
                order = ((32, 64, 96), (0, 128, 160))
            for h, (v, q, k) in enumerate(order):
                vt[h, :, at] = full[v : v + width]
                qt[h, :, at] = jnp.concatenate(
                    [full[q : q + width], apart], axis=0
                )
                kr[h, at, :] = jnp.concatenate([full[k : k + width], same], axis=0).T
    scale = 0.5 / math.sqrt(width)
    blocks = length // bq

    def low(qb):
        best = 0
        for edge in edges:
            best = jnp.where(qb * bq >= edge, edge, best)
        return best // bk

    def high(qb):
        return (qb + 1) * (bq // bk) - 1

    def count(qb, n):
        return n + high(qb) - low(qb) + 1

    tiles = lax.fori_loop(0, blocks, count, 0)

    ahead = lax.broadcasted_iota(jnp.int32, (bk, bq), 0) - lax.broadcasted_iota(
        jnp.int32, (bk, bq), 1
    )
    factor[0] = jnp.full((bk, bq), scale, f32)
    factor[1] = jnp.where(ahead <= 0, scale, 0.0)
    score = (score0, score1)
    weights = (weight0, weight1)

    def half_step(i, slot, now, then, past):
        qb, kb = then
        ends = (qb == kb).astype(jnp.int32)
        for h in range(head_groups):
            half = score[1 - slot][h] * factor[ends]
            weights[1 - slot][h] = (half * jnp.tanh(half) + half).astype(bf16)
        qb, kb = past
        q0 = pl.multiple_of(qb * bq, bq)
        k0 = pl.multiple_of(kb * bk, bk)
        device = q0 // tokens
        column = pl.multiple_of(q0 % tokens, bq)
        fresh = kb == low(qb)
        live = (i >= 2) & (i < tiles + 2)
        for h in range(head_groups):
            part = dot(vt[h, :, pl.ds(k0, bk)], weights[slot][h], 1, 0)
            part = jnp.where(live, part + jnp.where(fresh, 0.0, total[h]), total[h])
            total[h] = part
            out[device, h * width : (h + 1) * width, pl.ds(column, bq)] = part.astype(bf16)
        qb, kb = now
        q0 = pl.multiple_of(qb * bq, bq)
        k0 = pl.multiple_of(kb * bk, bk)
        for h in range(head_groups):
            score[slot][h] = dot(kr[h, pl.ds(k0, bk), :], qt[h, :, pl.ds(q0, bq)], 1, 0)
        done = kb == high(qb)
        last = done & (qb == blocks - 1)
        next_q = jnp.where(done & ~last, qb + 1, qb)
        next_k = jnp.where(last, kb, jnp.where(done, low(next_q), kb + 1))
        return next_q, next_k

    def step(j, state):
        now, then, past = state
        after = half_step(2 * j, 0, now, then, past)
        later = half_step(2 * j + 1, 1, after, now, then)
        return later, after, now

    start = (jnp.int32(0), jnp.int32(0))
    for ref in (score1, weight0):
        ref[...] = jnp.zeros(ref.shape, ref.dtype)
    total[...] = jnp.zeros(total.shape, f32)
    lax.fori_loop(0, (tiles + 3) // 2, step, (start, start, start))


def final_body(step, returned, carried_hbm, up_hbm, down_hbm, result, carried, up, down, out, sems):
    tokens, model = out.shape
    chunks = up.shape[1] // step
    places = (pl.ds(0, model), pl.ds(model + tokens, model), pl.ds(model, tokens))
    gate_load, out_load, embedded_load = [
        pltpu.make_async_copy(carried_hbm.at[at], carried.at[at], sems.at[i])
        for i, at in enumerate(places)
    ]
    ups = []
    downs = []
    for c in range(chunks):
        at = pl.ds(c * step, step)
        ups.append(pltpu.make_async_copy(up_hbm.at[:, at], up.at[:, at], sems.at[5 + 2 * c]))
        downs.append(pltpu.make_async_copy(down_hbm.at[at], down.at[at], sems.at[6 + 2 * c]))
    for load in (gate_load, out_load, embedded_load):
        load.start()
    for c in range(chunks):
        ups[c].start()
        downs[c].start()
    att = returned[...].astype(f32)
    att = att * rms(att, 0)
    gate_load.wait()
    heads = (att * carried[:model].astype(f32)).astype(bf16)
    out_load.wait()
    mixed = dot(heads, carried[model + tokens :], 0, 0)
    embedded_load.wait()
    hidden = carried[model : model + tokens].astype(f32) + mixed
    normed = (hidden * rms(hidden, 1)).astype(bf16)
    total = hidden
    for c in range(chunks):
        at = slice(c * step, (c + 1) * step)
        ups[c].wait()
        active = silu(dot(normed, up[:, at], 1, 0)).astype(bf16)
        downs[c].wait()
        if c + 1 < chunks:
            total = total + dot(active, down[at], 1, 0)
    saves = []
    half = tokens // 2
    for part in range(2):
        rows = slice(part * half, (part + 1) * half)
        out[rows] = (total[rows] + dot(active[rows], down[at], 1, 0)).astype(bf16)
        place = pl.ds(part * half, half)
        saves.append(pltpu.make_async_copy(out.at[place], result.at[place], sems.at[3 + part]))
        saves[-1].start()
    for save in saves:
        save.wait()


def local(
    token_rows,
    segment_ids,
    requests,
    hot_table,
    cold_table,
    input_weight,
    output_weight,
    up_weight,
    down_weight,
):
    both = ("emb", "seq")
    emb = lax.axis_size("emb")
    seq = lax.axis_size("seq")
    devices = emb * seq
    cap = requests.shape[2]
    hot, model = hot_table.shape
    tokens = token_rows.shape[1]
    groups = H // seq
    width = model // H
    own = lax.axis_index("seq")
    member = lax.axis_index("emb")
    span = seq * cap

    lines = tokens // LANES
    raw = cap * model // LANES
    message = call(
        message_body,
        jax.ShapeDtypeStruct((devices, lines + 2, LANES), jnp.int32),
        [VMEM] * 3,
        VMEM,
        name="message",
        size=60,
    )(token_rows, segment_ids, requests[0].T)
    heard = lax.all_to_all(message, both, split_axis=0, concat_axis=0, tiled=True)

    kept = LANES if groups == 1 else 192
    step = 512
    hot_projected = call(
        functools.partial(hot_body, groups, step),
        jax.ShapeDtypeStruct((kept, hot), bf16),
        [SMEM, HBM, HBM, HBM],
        HBM,
        [
            pltpu.VMEM((model, groups * 4 * width), bf16),
            pltpu.VMEM((hot, model), bf16),
            pltpu.VMEM((kept, hot), bf16),
            pltpu.SemaphoreType.DMA((2 * (hot // step) + 1,)),
        ],
        flops=2 * hot * model * 256,
        name="hot",
        size=60,
    )(own.astype(jnp.int32).reshape(1), message, input_weight, hot_table)

    span_lines = span if groups == 1 else span + span // 2
    sent = call(
        functools.partial(owner_body, groups, emb, seq, cap),
        jax.ShapeDtypeStruct((devices, span_lines + raw, LANES), bf16),
        [HBM, HBM, HBM, HBM],
        HBM,
        [
            pltpu.VMEM((devices, span_lines + raw, LANES), bf16),
            pltpu.VMEM((devices * cap * PICK, model), bf16),
            pltpu.VMEM(input_weight.shape, bf16),
            pltpu.SMEM((devices, LANES), jnp.int32),
            pltpu.VMEM((devices, LANES), jnp.int32),
            pltpu.SemaphoreType.DMA,
            pltpu.SemaphoreType.DMA,
            pltpu.SemaphoreType.DMA((2 + emb,)),
        ],
        flops=2 * devices * cap * model * 2048,
        name="owner",
        size=52,
    )(heard, cold_table, input_weight, hot_projected)
    got = lax.all_to_all(sent, both, split_axis=0, concat_axis=0, tiled=True)

    place = member.astype(jnp.int32).reshape(1)
    spread = call(
        functools.partial(spread_body, step, seq, lines),
        jax.ShapeDtypeStruct((kept, seq * tokens), bf16),
        [SMEM, VMEM, HBM],
        HBM,
        [
            pltpu.VMEM((step, tokens), jnp.int16),
            pltpu.VMEM((kept, hot), bf16),
            pltpu.VMEM((kept, seq * tokens), bf16),
            pltpu.SemaphoreType.DMA((seq + 1,)),
        ],
        flops=2 * seq * tokens * hot * 256,
        name="spread",
        size=51,
    )(place, heard, hot_projected)

    deep = width + 16
    tile = (groups, BK, BQ)
    attended = call(
        functools.partial(attend_body, groups, seq, cap, hot, width, BQ, BK, lines),
        jax.ShapeDtypeStruct((seq, groups * width, tokens), bf16),
        [SMEM, VMEM, HBM, VMEM],
        VMEM,
        [
            pltpu.VMEM((groups, deep, seq * tokens), bf16),
            pltpu.VMEM((groups, width, seq * tokens), bf16),
            pltpu.VMEM((groups, seq * tokens, deep), bf16),
            pltpu.VMEM(tile, f32),
            pltpu.VMEM(tile, f32),
            pltpu.VMEM(tile, bf16),
            pltpu.VMEM(tile, bf16),
            pltpu.VMEM((groups, width, BQ), f32),
            pltpu.VMEM((kept, seq * tokens), bf16),
            pltpu.VMEM((devices * 16, tokens), jnp.int16),
            pltpu.VMEM((2, BK, BQ), f32),
            pltpu.SemaphoreType.DMA((seq,)),
        ],
        flops=10**10,
        name="attend",
        size=51,
    )(place, heard, spread, got)
    returned = lax.all_to_all(attended, "seq", split_axis=0, concat_axis=0, tiled=True)

    carried = call(
        functools.partial(own_body, hot, cap, step),
        jax.ShapeDtypeStruct((2 * model + tokens, model), bf16),
        [VMEM, VMEM, HBM, HBM, HBM],
        HBM,
        [
            pltpu.VMEM((hot, model), bf16),
            pltpu.VMEM(input_weight.shape, bf16),
            pltpu.VMEM((tokens, model), bf16),
            pltpu.VMEM((model, tokens), bf16),
            pltpu.VMEM((model, model), bf16),
            pltpu.SemaphoreType.DMA((4 + hot // step,)),
        ],
        flops=2 * tokens * model * model,
        name="own",
        size=51,
    )(token_rows, got, hot_table, input_weight, output_weight)
    hidden_chunks = up_weight.shape[1] // step
    result = call(
        functools.partial(final_body, step),
        jax.ShapeDtypeStruct((tokens, model), bf16),
        [VMEM, HBM, HBM, HBM],
        HBM,
        [
            pltpu.VMEM((2 * model + tokens, model), bf16),
            pltpu.VMEM(up_weight.shape, bf16),
            pltpu.VMEM(down_weight.shape, bf16),
            pltpu.VMEM((tokens, model), bf16),
            pltpu.SemaphoreType.DMA((5 + 2 * hidden_chunks,)),
        ],
        flops=2 * tokens * model * 4096,
        name="final",
        size=52,
    )(returned.reshape(model, tokens), carried, up_weight, down_weight)
    return result[None]


BQ = 256
BK = 256


def solution(mesh):
    placed = (
        P("emb", "seq"),
        P("emb", "seq"),
        P(("emb", "seq"), None, None),
        P(),
        P(("emb", "seq"), None),
        P(),
        P(),
        P(),
        P(),
    )
    return jax.shard_map(
        local, mesh=mesh, in_specs=placed, out_specs=P("emb", "seq", None), check_vma=False
    )
```

```python
import functools
import math

import jax
import jax.numpy as jnp
from jax import lax
from jax.experimental import pallas as pl
from jax.experimental.pallas import tpu as pltpu
from jax.sharding import PartitionSpec as P

H = 16
LANES = 128
PICK = 8
SEGMENTS = 4
epsilon = 1e-06
APART = 2.0**30
f32 = jnp.float32
bf16 = jnp.bfloat16

VMEM = pl.BlockSpec(memory_space=pltpu.VMEM)
SMEM = pl.BlockSpec(memory_space=pltpu.SMEM)
HBM = pl.BlockSpec(memory_space=pl.ANY)


def call(body, out_shape, in_specs, out_specs, scratch=(), flops=0, name=None, size=60):
    return pl.pallas_call(
        body,
        out_shape=out_shape,
        in_specs=in_specs,
        out_specs=out_specs,
        scratch_shapes=list(scratch),
        compiler_params=pltpu.CompilerParams(vmem_limit_bytes=size * 1024 * 1024),
        cost_estimate=pl.CostEstimate(flops=flops, bytes_accessed=0, transcendentals=0),
        name=name,
    )


def dot(a, b, ca, cb):
    return lax.dot_general(a, b, (((ca,), (cb,)), ((), ())), preferred_element_type=f32)


def silu(x):
    half = x * 0.5
    return half * jnp.tanh(half) + half


def rms(x, axis):
    return lax.rsqrt(jnp.mean(x * x, axis=axis, keepdims=True) + epsilon)


def owner_body(
    head_groups, emb, seq, cap, message_hbm, cold, weight_hbm, after, sent_hbm,
    sent, tiles, weight, req, tags, sem, weight_sem, sems,
):
    count = emb * seq * cap
    per = LANES // cap
    span = seq * cap
    split = weight.shape[0] // LANES
    raw = cap * split
    load = pltpu.make_async_copy(weight_hbm, weight, weight_sem)

    wanted_line = message_hbm.shape[1] - 2
    asked = pltpu.make_async_copy(message_hbm.at[:, wanted_line, :], req, sems.at[0])
    asked.start()
    again = pltpu.make_async_copy(message_hbm.at[:, wanted_line, :], tags, sems.at[1])
    again.start()
    load.start()
    asked.wait()
    batch = 8

    def fetch(j, _):
        for i in range(batch):
            for k in range(cap):
                row = req[j * batch + i, k]
                base = pl.multiple_of((row // PICK) * PICK, PICK)
                slot = pl.multiple_of(((j * batch + i) * cap + k) * PICK, PICK)
                pltpu.make_async_copy(
                    cold.at[pl.ds(base, PICK)], tiles.at[pl.ds(slot, PICK)], sem
                ).start()
        return 0

    lax.fori_loop(0, emb * seq // batch, fetch, 0)
    again.wait()
    picks = []
    for group in range(count // LANES):
        owner = lax.broadcasted_iota(jnp.int32, (per, LANES), 0)
        lane = lax.broadcasted_iota(jnp.int32, (per, LANES), 1)
        mine = jnp.where(lane // cap == owner, tags[group * per : (group + 1) * per], 0)
        wanted = jnp.sum(mine, axis=0, keepdims=True)
        place = lax.broadcasted_iota(jnp.int32, (LANES * PICK, LANES), 0)
        column = lax.broadcasted_iota(jnp.int32, (1, LANES), 1)
        pick = (place == column * PICK + wanted % PICK).astype(f32)
        picks.append(pick.T.astype(bf16))
    line = lax.broadcasted_iota(jnp.int32, (per * raw, LANES), 0)
    source = lax.broadcasted_iota(jnp.int32, (per * raw, LANES), 1)
    repeat = ((line // raw) * cap + line % cap == source).astype(f32).astype(bf16)
    chunk = (lax.broadcasted_iota(jnp.int32, (per * raw, LANES), 0) % raw) // cap
    saves = []
    pltpu.make_async_copy(cold.at[pl.ds(0, count * PICK)], tiles, sem).wait()
    load.wait()
    for group in range(count // LANES):
        block = tiles[group * LANES * PICK : (group + 1) * LANES * PICK]
        part = dot(picks[group], block, 1, 0)
        normed = (part * rms(part, 1)).astype(bf16)
        projected = dot(normed, weight[...], 1, 0).astype(bf16)
        spread = dot(repeat, part.astype(bf16), 1, 0)
        lines = spread[:, :LANES]
        for c in range(1, split):
            lines = jnp.where(chunk == c, spread[:, c * LANES : (c + 1) * LANES], lines)
        kept = sent.shape[1] - raw
        sent[group * per : (group + 1) * per, kept:] = lines.astype(bf16).reshape(
            per, raw, LANES
        )
        for local in range(LANES // span):
            member = group * (LANES // span) + local
            for g in range(seq):
                piece = projected[local * span : (local + 1) * span]
                if head_groups == 1:
                    sent[member * seq + g, :span] = piece[:, g * LANES : (g + 1) * LANES]
                else:
                    low = piece[:, (2 * g) * LANES : (2 * g + 1) * LANES]
                    high = piece[:, (2 * g + 1) * LANES : (2 * g + 2) * LANES]
                    sent[member * seq + g, :span] = jnp.concatenate(
                        [high[:, 32:64], low[:, 32:]], axis=1
                    )
                    sent[member * seq + g, span:kept] = jnp.concatenate(
                        [high[span // 2 :, 64:], high[: span // 2, 64:]], axis=1
                    )
            at = pl.ds(member * seq, seq)
            saves.append(
                pltpu.make_async_copy(sent.at[at], sent_hbm.at[at], sems.at[2 + len(saves)])
            )
            saves[-1].start()
    for save in saves:
        save.wait()


def message_body(ids, segments, wanted, out):
    devices, lines, _ = out.shape
    cap = wanted.shape[0]
    lane = lax.broadcasted_iota(jnp.int32, (1, LANES), 1)
    edges = jnp.zeros((1, LANES), jnp.int32)
    for s in range(1, SEGMENTS):
        below = jnp.sum((segments[...] < s).astype(jnp.int32), axis=1, keepdims=True)
        edges = jnp.where(lane == s, below, edges)
    for j in range(lines - 2):
        out[:, j, :] = jnp.broadcast_to(
            ids[:, j * LANES : (j + 1) * LANES], (devices, LANES)
        )
    asked = wanted[...].astype(f32).T.astype(jnp.int32)
    tags = jnp.broadcast_to(asked[:, 0:1], (devices, LANES))
    for k in range(1, cap):
        tags = jnp.where(lane % cap == k, asked[:, k : k + 1], tags)
    out[:, lines - 2, :] = tags
    out[:, lines - 1, :] = jnp.broadcast_to(edges, (devices, LANES))


def hot_body(head_groups, step, own, after, weight_hbm, table_hbm, out_hbm, weight, table, out, sems):
    hot = table.shape[0]
    chunks = hot // step
    lanes = weight.shape[1]
    begin = pl.multiple_of(own[0] * lanes, lanes)
    first = pltpu.make_async_copy(
        weight_hbm.at[:, pl.ds(begin, lanes)], weight, sems.at[2 * chunks]
    )
    first.start()
    loads = [
        pltpu.make_async_copy(
            table_hbm.at[pl.ds(c * step, step)], table.at[pl.ds(c * step, step)], sems.at[c]
        )
        for c in range(chunks)
    ]
    saves = [
        pltpu.make_async_copy(
            out.at[:, pl.ds(c * step, step)],
            out_hbm.at[:, pl.ds(c * step, step)],
            sems.at[chunks + c],
        )
        for c in range(chunks)
    ]
    for load in loads:
        load.start()
    first.wait()
    wide = weight[...].astype(f32).T.astype(bf16)
    for c in range(chunks):
        at = slice(c * step, (c + 1) * step)
        loads[c].wait()
        x = table[at].astype(f32)
        normed = (x * rms(x, 1)).astype(bf16)
        flat = dot(wide, normed, 1, 1).astype(bf16)
        if head_groups == 1:
            out[:, at] = flat
        else:
            out[0:32, at] = flat[160:192]
            out[32:128, at] = flat[32:128]
            out[128:192, at] = flat[192:256]
        saves[c].start()
    for save in saves:
        save.wait()


def item_row(heard, at, lines):
    return jnp.concatenate([heard[at, j : j + 1, :] for j in range(lines)], axis=1)


def spread_body(step, seq, lines, member, heard, table_hbm, out_hbm, base, table, out, sems):
    tokens = lines * LANES
    hot = table.shape[1]
    load = pltpu.make_async_copy(table_hbm, table, sems.at[seq])
    load.start()
    base[...] = lax.broadcasted_iota(jnp.int32, base.shape, 0).astype(jnp.int16)
    load.wait()

    def save(s):
        column = pl.multiple_of(s * tokens, tokens)
        return pltpu.make_async_copy(
            out.at[:, pl.ds(column, tokens)], out_hbm.at[:, pl.ds(column, tokens)], sems.at[s]
        )

    def one(s, _):
        own = item_row(heard, member[0] * seq + s, lines)
        column = pl.multiple_of(s * tokens, tokens)
        acc = jnp.zeros((out.shape[0], tokens), f32)
        for c in range(hot // step):
            place = (own - c * step).astype(jnp.int16)
            pick = jnp.where(base[...] == place, jnp.ones((), bf16), jnp.zeros((), bf16))
            acc = acc + dot(table[:, c * step : (c + 1) * step], pick, 1, 0)
        out[:, pl.ds(column, tokens)] = acc.astype(bf16)
        save(s).start()
        return 0

    lax.fori_loop(0, seq, one, 0)
    for s in range(seq):
        save(s).wait()


def own_body(
    hot, cap, step, ids, got, table_hbm, weight_hbm, out_hbm, carried,
    table, weight, embedded, gates, out_weight, sems,
):
    tokens, model = embedded.shape
    chunks = hot // step
    loads = [
        pltpu.make_async_copy(
            table_hbm.at[pl.ds(c * step, step)], table.at[pl.ds(c * step, step)], sems.at[3 + c]
        )
        for c in range(chunks)
    ]
    for load in loads:
        load.start()
    load = pltpu.make_async_copy(weight_hbm, weight, sems.at[0])
    load.start()
    third = pltpu.make_async_copy(out_hbm, out_weight, sems.at[3 + chunks])
    third.start()
    items = jnp.broadcast_to(ids[...].astype(f32), (8, tokens)).T[:, 0:1].astype(jnp.int32)
    split = model // LANES
    raw = cap * split
    owners = got.shape[0]
    lines = got[:, got.shape[1] - raw :, :].reshape(owners * raw, LANES)
    slot = items - hot
    code = jnp.where(slot >= 0, (slot // cap) * raw + slot % cap, -raw)
    place = lax.broadcasted_iota(jnp.int32, (tokens, owners * raw), 1)
    parts = []
    for c in range(split):
        pick = (place == code + c * cap).astype(f32).astype(bf16)
        parts.append(dot(pick, lines, 1, 0))
    emb = jnp.concatenate(parts, axis=1)
    for c in range(chunks):
        loads[c].wait()
        place = lax.broadcasted_iota(jnp.int32, (tokens, step), 1) + c * step
        pick = (place == items).astype(f32).astype(bf16)
        emb = emb + dot(pick, table[c * step : (c + 1) * step], 1, 0)
    embedded[...] = emb.astype(bf16)
    save = pltpu.make_async_copy(embedded, carried.at[pl.ds(model, tokens)], sems.at[1])
    save.start()
    third.wait()
    third = pltpu.make_async_copy(
        out_weight, carried.at[pl.ds(model + tokens, model)], sems.at[3 + chunks]
    )
    third.start()
    normed = (emb * rms(emb, 1)).astype(bf16)
    load.wait()
    step = weight.shape[1] // H
    width = model // H
    wide = jnp.concatenate(
        [
            weight[:, h * step : (h + 1) * step].astype(f32).T[:width]
            for h in range(H)
        ],
        axis=0,
    ).astype(bf16)
    u = dot(wide, normed, 1, 1).astype(bf16).astype(f32)
    gates[...] = silu(u).astype(bf16)
    other = pltpu.make_async_copy(gates, carried.at[pl.ds(0, model)], sems.at[2])
    other.start()
    save.wait()
    third.wait()
    other.wait()


def attend_body(
    head_groups, seq, cap, hot, width, bq, bk, lines, member, heard, table, got, out_hbm,
    out, qt, vt, kr, score0, score1, weight0, weight1, total, base, factor, out_sems
):
    tokens = lines * LANES
    length = seq * tokens
    owners = got.shape[0]
    quarter = 16 // cap
    span = seq * cap
    depth = qt.shape[1]
    kept = span if head_groups == 1 else span + span // 2
    mine = heard[pl.ds(member[0] * seq, seq), lines + 1, :]
    lane = lax.broadcasted_iota(jnp.int32, mine.shape, 1)
    edges = [jnp.sum(jnp.where(lane == i, mine, 0)) for i in range(1, SEGMENTS)]
    base[...] = lax.broadcasted_iota(jnp.int32, base.shape, 0).astype(jnp.int16)
    for part in range(span // 16):
        a = got[:, part * 16 : (part + 1) * 16, :].reshape(owners * 16, LANES)
        if head_groups == 1:
            lhs = a.astype(f32).T.astype(bf16)
        else:
            b = got[:, span:kept, :].reshape(owners * 16, LANES).astype(f32).T
            b = b[64:] if part == 0 else b[:64]
            lhs = jnp.concatenate([a.astype(f32).T, b], axis=0).astype(bf16)
        for within in range(quarter):
            s = part * quarter + within
            slot = item_row(heard, member[0] * seq + s, lines) - hot
            code = jnp.where(slot >= 0, (slot // cap) * 16 + within * cap + slot % cap, -1)
            pick = jnp.where(
                base[...] == code.astype(jnp.int16), jnp.ones((), bf16), jnp.zeros((), bf16)
            )
            at = slice(s * tokens, (s + 1) * tokens)
            full = dot(lhs, pick, 1, 0).astype(bf16) + table[:, at]
            spot = s * tokens + lax.broadcasted_iota(jnp.int32, (1, tokens), 1)
            segment = jnp.zeros((1, tokens), jnp.int32)
            for edge in edges:
                segment = segment + (spot >= edge).astype(jnp.int32)
            level = lax.broadcasted_iota(jnp.int32, (depth - width, tokens), 0)
            same = (level == segment).astype(f32)
            apart = ((same - 1.0) * APART).astype(bf16)
            same = same.astype(bf16)
            if head_groups == 1:
                order = ((32, 64, 96),)
            else:
                order = ((32, 64, 96), (0, 128, 160))
            for h, (v, q, k) in enumerate(order):
                vt[h, :, at] = full[v : v + width]
                qt[h, :, at] = jnp.concatenate(
                    [full[q : q + width], apart], axis=0
                )
                kr[h, at, :] = jnp.concatenate([full[k : k + width], same], axis=0).T
    scale = 0.5 / math.sqrt(width)
    blocks = length // bq

    def low(qb):
        best = 0
        for edge in edges:
            best = jnp.where(qb * bq >= edge, edge, best)
        return best // bk

    def high(qb):
        return (qb + 1) * (bq // bk) - 1

    def count(qb, n):
        return n + high(qb) - low(qb) + 1

    tiles = lax.fori_loop(0, blocks, count, 0)

    ahead = lax.broadcasted_iota(jnp.int32, (bk, bq), 0) - lax.broadcasted_iota(
        jnp.int32, (bk, bq), 1
    )
    factor[0] = jnp.full((bk, bq), scale, f32)
    factor[1] = jnp.where(ahead <= 0, scale, 0.0)
    score = (score0, score1)
    weights = (weight0, weight1)

    def half_step(i, slot, now, then, past):
        qb, kb = then
        ends = (qb == kb).astype(jnp.int32)
        for h in range(head_groups):
            half = score[1 - slot][h] * factor[ends]
            weights[1 - slot][h] = (half * jnp.tanh(half) + half).astype(bf16)
        qb, kb = past
        q0 = pl.multiple_of(qb * bq, bq)
        k0 = pl.multiple_of(kb * bk, bk)
        device = q0 // tokens
        column = pl.multiple_of(q0 % tokens, bq)
        fresh = kb == low(qb)
        live = (i >= 2) & (i < tiles + 2)
        for h in range(head_groups):
            part = dot(vt[h, :, pl.ds(k0, bk)], weights[slot][h], 1, 0)
            part = jnp.where(live, part + jnp.where(fresh, 0.0, total[h]), total[h])
            total[h] = part
            out[device, h * width : (h + 1) * width, pl.ds(column, bq)] = part.astype(bf16)
        qb, kb = now
        q0 = pl.multiple_of(qb * bq, bq)
        k0 = pl.multiple_of(kb * bk, bk)
        for h in range(head_groups):
            score[slot][h] = dot(kr[h, pl.ds(k0, bk), :], qt[h, :, pl.ds(q0, bq)], 1, 0)
        done = kb == high(qb)
        last = done & (qb == blocks - 1)
        next_q = jnp.where(done & ~last, qb + 1, qb)
        next_k = jnp.where(last, kb, jnp.where(done, low(next_q), kb + 1))
        return next_q, next_k

    def leave(device):
        return pltpu.make_async_copy(out.at[device], out_hbm.at[device], out_sems.at[device])

    def finish(i, tile):
        qb, kb = tile
        live = (i >= 2) & (i < tiles + 2)
        ended = ((qb + 1) * bq) % tokens == 0

        @pl.when(live & ended & (kb == high(qb)))
        def _():
            leave(qb * bq // tokens).start()

    def step(j, state):
        now, then, past = state
        after = half_step(2 * j, 0, now, then, past)
        later = half_step(2 * j + 1, 1, after, now, then)
        finish(2 * j, past)
        finish(2 * j + 1, then)
        return later, after, now

    start = (jnp.int32(0), jnp.int32(0))
    for ref in (score1, weight0):
        ref[...] = jnp.zeros(ref.shape, ref.dtype)
    total[...] = jnp.zeros(total.shape, f32)
    lax.fori_loop(0, (tiles + 3) // 2, step, (start, start, start))
    for device in range(seq):
        leave(device).wait()


def final_body(step, returned, carried_hbm, up_hbm, down_hbm, result, carried, up, down, out, sems):
    tokens, model = out.shape
    chunks = up.shape[1] // step
    places = (pl.ds(0, model), pl.ds(model + tokens, model), pl.ds(model, tokens))
    gate_load, out_load, embedded_load = [
        pltpu.make_async_copy(carried_hbm.at[at], carried.at[at], sems.at[i])
        for i, at in enumerate(places)
    ]
    ups = []
    downs = []
    for c in range(chunks):
        at = pl.ds(c * step, step)
        ups.append(pltpu.make_async_copy(up_hbm.at[:, at], up.at[:, at], sems.at[5 + 2 * c]))
        downs.append(pltpu.make_async_copy(down_hbm.at[at], down.at[at], sems.at[6 + 2 * c]))
    for load in (gate_load, out_load, embedded_load):
        load.start()
    for c in range(chunks):
        ups[c].start()
        downs[c].start()
    att = returned[...].astype(f32)
    att = att * rms(att, 0)
    gate_load.wait()
    heads = (att * carried[:model].astype(f32)).astype(bf16)
    out_load.wait()
    mixed = dot(heads, carried[model + tokens :], 0, 0)
    embedded_load.wait()
    hidden = carried[model : model + tokens].astype(f32) + mixed
    normed = (hidden * rms(hidden, 1)).astype(bf16)
    total = hidden
    for c in range(chunks):
        at = slice(c * step, (c + 1) * step)
        ups[c].wait()
        active = silu(dot(normed, up[:, at], 1, 0)).astype(bf16)
        downs[c].wait()
        if c + 1 < chunks:
            total = total + dot(active, down[at], 1, 0)
    saves = []
    half = tokens // 2
    for part in range(2):
        rows = slice(part * half, (part + 1) * half)
        out[rows] = (total[rows] + dot(active[rows], down[at], 1, 0)).astype(bf16)
        place = pl.ds(part * half, half)
        saves.append(pltpu.make_async_copy(out.at[place], result.at[place], sems.at[3 + part]))
        saves[-1].start()
    for save in saves:
        save.wait()


def local(
    token_rows,
    segment_ids,
    requests,
    hot_table,
    cold_table,
    input_weight,
    output_weight,
    up_weight,
    down_weight,
):
    both = ("emb", "seq")
    emb = lax.axis_size("emb")
    seq = lax.axis_size("seq")
    devices = emb * seq
    cap = requests.shape[2]
    hot, model = hot_table.shape
    tokens = token_rows.shape[1]
    groups = H // seq
    width = model // H
    own = lax.axis_index("seq")
    member = lax.axis_index("emb")
    span = seq * cap

    lines = tokens // LANES
    raw = cap * model // LANES
    message = call(
        message_body,
        jax.ShapeDtypeStruct((devices, lines + 2, LANES), jnp.int32),
        [VMEM] * 3,
        VMEM,
        name="message",
        size=60,
    )(token_rows, segment_ids, requests[0].T)
    heard = lax.all_to_all(message, both, split_axis=0, concat_axis=0, tiled=True)

    kept = LANES if groups == 1 else 192
    step = 512
    hot_projected = call(
        functools.partial(hot_body, groups, step),
        jax.ShapeDtypeStruct((kept, hot), bf16),
        [SMEM, HBM, HBM, HBM],
        HBM,
        [
            pltpu.VMEM((model, groups * 4 * width), bf16),
            pltpu.VMEM((hot, model), bf16),
            pltpu.VMEM((kept, hot), bf16),
            pltpu.SemaphoreType.DMA((2 * (hot // step) + 1,)),
        ],
        flops=2 * hot * model * 256,
        name="hot",
        size=60,
    )(own.astype(jnp.int32).reshape(1), message, input_weight, hot_table)

    span_lines = span if groups == 1 else span + span // 2
    sent = call(
        functools.partial(owner_body, groups, emb, seq, cap),
        jax.ShapeDtypeStruct((devices, span_lines + raw, LANES), bf16),
        [HBM, HBM, HBM, HBM],
        HBM,
        [
            pltpu.VMEM((devices, span_lines + raw, LANES), bf16),
            pltpu.VMEM((devices * cap * PICK, model), bf16),
            pltpu.VMEM(input_weight.shape, bf16),
            pltpu.SMEM((devices, LANES), jnp.int32),
            pltpu.VMEM((devices, LANES), jnp.int32),
            pltpu.SemaphoreType.DMA,
            pltpu.SemaphoreType.DMA,
            pltpu.SemaphoreType.DMA((2 + emb,)),
        ],
        flops=2 * devices * cap * model * 2048,
        name="owner",
        size=52,
    )(heard, cold_table, input_weight, hot_projected)
    got = lax.all_to_all(sent, both, split_axis=0, concat_axis=0, tiled=True)

    place = member.astype(jnp.int32).reshape(1)
    spread = call(
        functools.partial(spread_body, step, seq, lines),
        jax.ShapeDtypeStruct((kept, seq * tokens), bf16),
        [SMEM, VMEM, HBM],
        HBM,
        [
            pltpu.VMEM((step, tokens), jnp.int16),
            pltpu.VMEM((kept, hot), bf16),
            pltpu.VMEM((kept, seq * tokens), bf16),
            pltpu.SemaphoreType.DMA((seq + 1,)),
        ],
        flops=2 * seq * tokens * hot * 256,
        name="spread",
        size=51,
    )(place, heard, hot_projected)

    deep = width + 16
    tile = (groups, BK, BQ)
    attended = call(
        functools.partial(attend_body, groups, seq, cap, hot, width, BQ, BK, lines),
        jax.ShapeDtypeStruct((seq, groups * width, tokens), bf16),
        [SMEM, VMEM, VMEM, VMEM],
        HBM,
        [
            pltpu.VMEM((seq, groups * width, tokens), bf16),
            pltpu.VMEM((groups, deep, seq * tokens), bf16),
            pltpu.VMEM((groups, width, seq * tokens), bf16),
            pltpu.VMEM((groups, seq * tokens, deep), bf16),
            pltpu.VMEM(tile, f32),
            pltpu.VMEM(tile, f32),
            pltpu.VMEM(tile, bf16),
            pltpu.VMEM(tile, bf16),
            pltpu.VMEM((groups, width, BQ), f32),
            pltpu.VMEM((devices * 16, tokens), jnp.int16),
            pltpu.VMEM((2, BK, BQ), f32),
            pltpu.SemaphoreType.DMA((seq,)),
        ],
        flops=10**10,
        name="attend",
        size=51,
    )(place, heard, spread, got)
    returned = lax.all_to_all(attended, "seq", split_axis=0, concat_axis=0, tiled=True)

    carried = call(
        functools.partial(own_body, hot, cap, step),
        jax.ShapeDtypeStruct((2 * model + tokens, model), bf16),
        [VMEM, VMEM, HBM, HBM, HBM],
        HBM,
        [
            pltpu.VMEM((hot, model), bf16),
            pltpu.VMEM(input_weight.shape, bf16),
            pltpu.VMEM((tokens, model), bf16),
            pltpu.VMEM((model, tokens), bf16),
            pltpu.VMEM((model, model), bf16),
            pltpu.SemaphoreType.DMA((4 + hot // step,)),
        ],
        flops=2 * tokens * model * model,
        name="own",
        size=51,
    )(token_rows, got, hot_table, input_weight, output_weight)
    hidden_chunks = up_weight.shape[1] // step
    result = call(
        functools.partial(final_body, step),
        jax.ShapeDtypeStruct((tokens, model), bf16),
        [VMEM, HBM, HBM, HBM],
        HBM,
        [
            pltpu.VMEM((2 * model + tokens, model), bf16),
            pltpu.VMEM(up_weight.shape, bf16),
            pltpu.VMEM(down_weight.shape, bf16),
            pltpu.VMEM((tokens, model), bf16),
            pltpu.SemaphoreType.DMA((5 + 2 * hidden_chunks,)),
        ],
        flops=2 * tokens * model * 4096,
        name="final",
        size=52,
    )(returned.reshape(model, tokens), carried, up_weight, down_weight)
    return result[None]


BQ = 256
BK = 256


def solution(mesh):
    placed = (
        P("emb", "seq"),
        P("emb", "seq"),
        P(("emb", "seq"), None, None),
        P(),
        P(("emb", "seq"), None),
        P(),
        P(),
        P(),
        P(),
    )
    return jax.shard_map(
        local, mesh=mesh, in_specs=placed, out_specs=P("emb", "seq", None), check_vma=False
    )
```
